128 devices in a mesh: row: 8 (over x, y_lo), col: 16 (over y_hi, z, core).
Axes of the slice: x: 4, y: 4 (y_hi: 2, y_lo: 2; y = y_hi * 2 + y_lo), z: 4, core: 2. Of those that a mesh axis runs over, the one named last changes fastest.
Arguments:
- h_old: float32 [8, 16, 1024, 2048], P('row', 'col'), may hold values from -2 to 2, as said below
- s_old: float32 [8, 16, 1024, 64], P('row', 'col'), may hold values from -100 to 100, as said below
- row_owner: int32 [256], replicated, may hold values from 0 to 15, as said below
- col_owner: int32 [256], replicated, may hold values from 0 to 7, as said below
Outputs:
- h_reduced: float32 [16384, 16384], P('row', 'col')
- panel_factor: float32 [16384, 512], P('row')
The draws below stay inside these ranges and needn't reach their ends.
Inputs may be any that keep to these rules, and one draw needn't show every extreme that they name: `row_owner`: each aligned run of 16 entries is an ordering of 0 to 15. `col_owner`: each aligned run of 8 entries is an ordering of 0 to 7. `s_old`: the first 512 rows of S_panel form a symmetric positive definite matrix. `h_old`: H is symmetric.
All inputs are finite; a program needn't handle non-finite values.
Results may differ from the reference program's by a relative error of at most 0.00017.
Values sent between devices are 32-bit elements; how exact they have to be, the bound alone decides.
A program may use at most 192 MiB of HBM per device.

```python
from functools import partial
import jax
import jax.numpy as jnp
from jax import lax

ORDER = 16384
PANEL = 512
BLOCK = 64
OLD_ROWS = 16
OLD_COLS = 8
N_ROW = 8
N_COL = 16


def shuffled(subkey, count):
    return jax.random.permutation(subkey, count)


def owner_maps(key):
    base = jax.random.fold_in(key, 7001)
    row_keys = jax.random.split(jax.random.fold_in(base, 1), ORDER // (BLOCK * OLD_ROWS))
    col_keys = jax.random.split(jax.random.fold_in(base, 2), ORDER // (BLOCK * OLD_COLS))
    rows = jax.vmap(partial(shuffled, count=OLD_ROWS))(row_keys).reshape(-1).astype(jnp.int32)
    cols = jax.vmap(partial(shuffled, count=OLD_COLS))(col_keys).reshape(-1).astype(jnp.int32)
    return (rows, cols)


def to_layout(natural, owner_rows, owner_cols):
    blocks_row = natural.shape[0] // BLOCK
    blocks_col = natural.shape[1] // BLOCK
    tiles = natural.reshape(blocks_row, BLOCK, blocks_col, BLOCK).transpose(0, 2, 1, 3)
    owner_row = owner_rows[:blocks_row][:, None]
    owner_col = owner_cols[:blocks_col][None, :]
    shape_two = (blocks_row, blocks_col)
    device_row = jnp.broadcast_to(owner_row // 2, shape_two)
    device_col = 2 * owner_col + owner_row % 2
    slot_row = jnp.broadcast_to((jnp.arange(blocks_row, dtype=jnp.int32) // OLD_ROWS)[:, None], shape_two)
    slot_col = jnp.broadcast_to((jnp.arange(blocks_col, dtype=jnp.int32) // OLD_COLS)[None, :], shape_two)
    stored = jnp.zeros((OLD_ROWS // 2, OLD_COLS * 2, blocks_row // OLD_ROWS, blocks_col // OLD_COLS, BLOCK, BLOCK), jnp.float32)
    stored = stored.at[device_row, device_col, slot_row, slot_col].set(tiles)
    return stored.transpose(0, 1, 2, 4, 3, 5).reshape(OLD_ROWS // 2, OLD_COLS * 2, blocks_row // OLD_ROWS * BLOCK, blocks_col // OLD_COLS * BLOCK)


def draw_row_owner(key, part):
    return owner_maps(key)[0]


def draw_col_owner(key, part):
    return owner_maps(key)[1]


def draw_h_old(key, part):
    owner_rows, owner_cols = owner_maps(key)
    subkey = jax.random.fold_in(key, 11)
    noise = jax.random.truncated_normal(subkey, -6.0, 6.0, (ORDER, ORDER), jnp.float32)
    natural = (noise + noise.T) * 0.15
    return to_layout(natural, owner_rows, owner_cols)


def draw_s_old(key, part):
    owner_rows, owner_cols = owner_maps(key)
    square = jax.random.truncated_normal(jax.random.fold_in(key, 21), -6.0, 6.0, (PANEL, PANEL), jnp.float32)
    diagonal = jax.random.uniform(jax.random.fold_in(key, 22), (PANEL,), jnp.float32, 3.0, 5.0)
    corner = (square + square.T) / jnp.sqrt(2.0 * PANEL) + jnp.diag(diagonal)
    below = 0.5 * jax.random.truncated_normal(jax.random.fold_in(key, 23), -6.0, 6.0, (ORDER - PANEL, PANEL), jnp.float32)
    natural = jnp.concatenate([corner, below], 0)
    return to_layout(natural, owner_rows, owner_cols)


def setup_inputs(seed: int = 0) -> dict:
    key_of = jax.random.split(jax.random.key(seed), 5)
    h_old = draw_h_old(jax.random.fold_in(key_of[4], 71), 0)
    s_old = draw_s_old(jax.random.fold_in(key_of[4], 71), 0)
    row_owner = draw_row_owner(jax.random.fold_in(key_of[4], 71), 0)
    col_owner = draw_col_owner(jax.random.fold_in(key_of[4], 71), 0)
    return dict(h_old=h_old, s_old=s_old, row_owner=row_owner, col_owner=col_owner)


def from_layout(stored, owner_rows, owner_cols, blocks_col):
    blocks_row = owner_rows.shape[0]
    grid = stored.reshape(N_ROW, N_COL, stored.shape[2] // BLOCK, BLOCK, stored.shape[3] // BLOCK, BLOCK)
    owner_row = owner_rows[:, None]
    owner_col = owner_cols[:blocks_col][None, :]
    shape_two = (blocks_row, blocks_col)
    device_row = jnp.broadcast_to(owner_row // 2, shape_two)
    device_col = 2 * owner_col + owner_row % 2
    slot_row = jnp.broadcast_to((jnp.arange(blocks_row, dtype=jnp.int32) // OLD_ROWS)[:, None], shape_two)
    slot_col = jnp.broadcast_to((jnp.arange(blocks_col, dtype=jnp.int32) // OLD_COLS)[None, :], shape_two)
    picked = grid[device_row, device_col, slot_row, :, slot_col, :]
    return picked.transpose(0, 2, 1, 3).reshape(blocks_row * BLOCK, blocks_col * BLOCK)

def reference(h_old, s_old, row_owner, col_owner):
    h_full = from_layout(h_old, row_owner, col_owner, ORDER // BLOCK)
    s_panel = from_layout(s_old, row_owner, col_owner, PANEL // BLOCK)
    lower_factor = jnp.linalg.cholesky(s_panel[:PANEL])
    solved = lax.linalg.triangular_solve(lower_factor, s_panel.T, left_side=True, lower=True)
    panel_factor = solved.T
    coupling = lax.linalg.triangular_solve(lower_factor, solved, left_side=True, lower=True, transpose_a=True).T
    identity = jnp.eye(PANEL, dtype=jnp.float32)
    inverse = lax.linalg.triangular_solve(lower_factor, identity, left_side=True, lower=True)
    coupling = coupling.at[:PANEL].set(identity - inverse)
    h_panel = h_full[:, :PANEL]
    mixed = h_panel - 0.5 * jnp.dot(coupling, h_panel[:PANEL], precision=lax.Precision.HIGHEST)
    left_terms = jnp.concatenate([coupling, mixed], 1)
    right_terms = jnp.concatenate([mixed, coupling], 1)
    update = jnp.dot(left_terms, right_terms.T, precision=lax.Precision.HIGHEST)
    return (h_full - update, panel_factor)
```

```python
import jax
import jax.numpy as jnp
from jax import lax
from jax.experimental import pallas as pl
from jax.experimental.pallas import tpu as pltpu
from jax.sharding import PartitionSpec as P

ORDER = 16384
PANEL = 512
BLOCK = 64
STEP = 128
HIGHEST = lax.Precision.HIGHEST
BF16 = jnp.bfloat16
F32 = jnp.float32


def dot(a, b, ca, cb, precision=None):
    return lax.dot_general(
        a, b, (((ca,), (cb,)), ((), ())), precision=precision, preferred_element_type=F32
    )


def halves(x):
    high = x.astype(BF16)
    return high, (x - high.astype(F32)).astype(BF16)


def lower_half(shape):
    return lax.broadcasted_iota(jnp.int32, shape, 1) < BLOCK


def fetch_panel(read, rows, first, row_owner, col_owner, s_out, h_out):
    low = lower_half((BLOCK, 2 * BLOCK))
    for i in range(rows):
        p = row_owner[first + i]
        for k in range(0, PANEL // BLOCK, 2):
            one = read(i, p, col_owner[k])
            two = read(i, p, col_owner[k + 1])
            at = (pl.ds(i * BLOCK, BLOCK), pl.ds(k * BLOCK, 2 * BLOCK))
            s_out[at] = jnp.where(low, one, pltpu.roll(two, BLOCK, 1))
            h_out[at] = jnp.where(low, pltpu.roll(one, BLOCK, 1), two)


def spread(x, rows):
    return jnp.broadcast_to(x, (rows, x.shape[1]))


def factor_inverse(a_ref, b_ref):
    sub = lax.broadcasted_iota(jnp.int32, (8, STEP), 0)
    for j in range(0, STEP, 8):
        far = STEP - j - 8
        a_near, b_near = a_ref[j : j + 8, :], b_ref[j : j + 8, :]
        near = [jnp.broadcast_to(a_near[:, j + t : j + t + 1], (8, STEP)) for t in range(8)]
        if far:
            a_far, b_far = a_ref[j + 8 :, :], b_ref[j + 8 :, :]
            cols = [jnp.broadcast_to(a_far[:, j + t : j + t + 1], (far, STEP)) for t in range(8)]
        scales, links = [], []
        for t in range(8):
            r = lax.rsqrt(near[t][t : t + 1, :])
            l = near[t] * spread(r, 8)
            below = jnp.where(sub > t, l, 0.0)
            a_row, b_row = a_near[t : t + 1, :] * r, b_near[t : t + 1, :] * r
            a_near = jnp.where(sub == t, spread(a_row, 8), a_near - below * spread(a_row, 8))
            b_near = jnp.where(sub == t, spread(b_row, 8), b_near - below * spread(b_row, 8))
            link = {}
            for u in range(t + 1, 8):
                link[u] = l[u : u + 1, :]
                near[u] = near[u] - l * spread(link[u], 8)
            scales.append(r)
            links.append(link)
        b_ref[j : j + 8, :] = b_near
        if far:
            for t in range(8):
                l = cols[t] * spread(scales[t], far)
                for u in range(t + 1, 8):
                    cols[u] = cols[u] - l * spread(links[t][u], far)
                a_far = a_far - l * spread(a_near[t : t + 1, :], far)
                b_far = b_far - l * spread(b_near[t : t + 1, :], far)
            a_ref[j + 8 :, :] = a_far
            b_ref[j + 8 :, :] = b_far


def corner_kernel(row_owner, col_owner, tiles, inverse, corner_h, s_top, work, a_blk, b_blk):
    fetch_panel(
        lambda i, p, q: tiles[2 * q + p % 2, p // 2],
        PANEL // BLOCK, 0, row_owner, col_owner, s_top, corner_h,
    )
    eye = lax.broadcasted_iota(jnp.int32, (STEP, STEP), 0) == lax.broadcasted_iota(
        jnp.int32, (STEP, STEP), 1
    )
    eye = jnp.where(eye, 1.0, 0.0)
    count = PANEL // STEP
    for k in range(count):
        work[k, :, :PANEL] = s_top[k * STEP : (k + 1) * STEP, :]
        work[k, :, PANEL:] = jnp.zeros((STEP, PANEL), F32)
        work[k, :, PANEL + k * STEP : PANEL + (k + 1) * STEP] = eye
    lane = lax.broadcasted_iota(jnp.int32, (STEP, PANEL), 1)

    def step(k, carry):
        a_blk[...] = work[k, :, pl.ds(pl.multiple_of(k * STEP, STEP), STEP)]
        b_blk[...] = eye
        factor_inverse(a_blk, b_blk)
        rows = dot(b_blk[...], work[k], 1, 0, HIGHEST)
        work[k] = rows
        ahead = jnp.where(lane >= (k + 1) * STEP, rows[:, :PANEL], 0.0).T
        for i in range(1, count):
            work[i] = work[i] - dot(ahead[i * STEP : (i + 1) * STEP], rows, 1, 0, HIGHEST)
        return carry

    lax.fori_loop(0, count, step, 0)
    for k in range(count):
        inverse[k * STEP : (k + 1) * STEP, :] = work[k, :, PANEL:]


def coupling_of(s_rows, inverse, special):
    factor = dot(s_rows, inverse, 1, 1, HIGHEST)
    coupling = dot(factor, inverse, 1, 0, HIGHEST)
    shape = (PANEL, PANEL)
    eye = lax.broadcasted_iota(jnp.int32, shape, 0) == lax.broadcasted_iota(jnp.int32, shape, 1)
    return factor, jnp.where(special, jnp.where(eye, 1.0, 0.0) - inverse, coupling)


def strip_kernel(place, row_owner, col_owner, tiles, inv, corner_h, high, low, s_buf, h_buf):
    step = pl.program_id(0)
    here = place[1]
    fetch_panel(
        lambda i, p, q: tiles[p // 2, 2 * q + p % 2],
        PANEL // BLOCK, here * 16 + step * 8, row_owner, col_owner, s_buf, h_buf,
    )
    special = jnp.logical_and(here == 0, step == 0)
    _, coupling = coupling_of(s_buf[...], inv[...], special)
    rest = h_buf[...] - dot(coupling, corner_h[...], 1, 0, HIGHEST)
    high[:, :PANEL], low[:, :PANEL] = halves(rest)
    high[:, PANEL:], low[:, PANEL:] = halves(coupling)


def band_kernel(place, row_owner, col_owner, tiles, inv, factor, high, low, s_buf, h_buf):
    step = pl.program_id(0)
    here = place[0]
    slot = pl.multiple_of((step // 2) * BLOCK, BLOCK)
    fetch_panel(
        lambda i, p, q: tiles[2 * q + p % 2, p // 2, pl.ds(slot, BLOCK), :],
        PANEL // BLOCK, here * 32 + step * 8, row_owner, col_owner, s_buf, h_buf,
    )
    special = jnp.logical_and(here == 0, step == 0)
    factor[...], coupling = coupling_of(s_buf[...], inv[...], special)
    high[:, :PANEL], low[:, :PANEL] = halves(coupling)
    high[:, PANEL:], low[:, PANEL:] = halves(h_buf[...])


def final_kernel(place, row_owner, col_owner, tiles, lh, ll, rh, rl, out):
    step = pl.program_id(0)
    blocks = out.shape[0] // BLOCK
    update = dot(lh[...], rh[...], 1, 1)
    update = update + dot(lh[...], rl[...], 1, 1)
    update = update + dot(ll[...], rh[...], 1, 1)
    out[...] = update
    low = lower_half((BLOCK, 2 * BLOCK))
    slot = pl.multiple_of((step * blocks // 16) * BLOCK, BLOCK)
    for i in range(blocks):
        p = row_owner[place[0] * 32 + step * blocks + i]
        for j in range(0, 16, 2):
            one = tiles[p // 2, 2 * col_owner[place[1] * 16 + j] + p % 2, pl.ds(slot, BLOCK), :]
            two = tiles[p // 2, 2 * col_owner[place[1] * 16 + j + 1] + p % 2, pl.ds(slot, BLOCK), :]
            if j < 8:
                both = jnp.where(low, one, pltpu.roll(two, BLOCK, 1))
            else:
                both = jnp.where(low, pltpu.roll(one, BLOCK, 1), two)
            at = (pl.ds(i * BLOCK, BLOCK), pl.ds(j * BLOCK, 2 * BLOCK))
            out[at] = both - out[at]


def whole(shape):
    return pl.BlockSpec(shape, lambda *i: (0,) * len(shape), pipeline_mode=pl.Buffered(1))


SMEM = pl.BlockSpec(memory_space=pltpu.SMEM)
LIMIT = pltpu.CompilerParams(vmem_limit_bytes=60 * 2**20)


def shape_of(shape, dtype=F32):
    return jax.ShapeDtypeStruct(shape, dtype)


def per_device(h_old, s_old, row_owner, col_owner):
    rows_n = lax.axis_size("row")
    cols_n = lax.axis_size("col")
    row_id = lax.axis_index("row")
    col_id = lax.axis_index("col")
    place = jnp.stack([row_id, col_id]).astype(jnp.int32)
    local_h = h_old[0, 0]
    local_s = s_old[0, 0]
    band = ORDER // rows_n
    strip = ORDER // cols_n
    panels = jnp.concatenate([local_s, local_h[:, :BLOCK]], axis=1)

    top = lax.all_gather(panels[:BLOCK], "row", axis=0)
    top = lax.all_gather(top, "col", axis=0)
    inverse, corner_h = pl.pallas_call(
        corner_kernel,
        out_shape=(shape_of((PANEL, PANEL)), shape_of((PANEL, PANEL))),
        in_specs=[SMEM, SMEM, pl.BlockSpec(memory_space=pltpu.VMEM)],
        scratch_shapes=[
            pltpu.VMEM((PANEL, PANEL), F32),
            pltpu.VMEM((PANEL // STEP, STEP, 2 * PANEL), F32),
            pltpu.VMEM((STEP, STEP), F32),
            pltpu.VMEM((STEP, STEP), F32),
        ],
        compiler_params=LIMIT,
        cost_estimate=pl.CostEstimate(flops=3 * 10**10, bytes_accessed=6 * 2**20, transcendentals=0),
        name="corner",
    )(row_owner, col_owner, top)

    band_tiles = lax.all_to_all(panels.reshape(rows_n, 128, 128), "row", 0, 0, tiled=True)
    band_tiles = lax.all_gather(band_tiles, "col", axis=0)
    strip_tiles = lax.all_to_all(panels.reshape(cols_n, BLOCK, 128), "col", 0, 0, tiled=True)
    strip_tiles = lax.all_gather(strip_tiles, "row", axis=0)

    outgoing = local_h.reshape(rows_n, 128, cols_n, 128).transpose(0, 2, 1, 3)
    h_tiles = lax.all_to_all(
        outgoing.reshape(rows_n * cols_n, 128, 128), ("row", "col"), 0, 0, tiled=True
    ).reshape(rows_n, cols_n, 128, 128)

    buffers = [pltpu.VMEM((PANEL, PANEL), F32), pltpu.VMEM((PANEL, PANEL), F32)]
    right_high, right_low = pl.pallas_call(
        strip_kernel,
        grid=(strip // PANEL,),
        out_shape=(shape_of((strip, 2 * PANEL), BF16),) * 2,
        in_specs=[SMEM, SMEM, SMEM, whole(strip_tiles.shape), whole((PANEL, PANEL)), whole((PANEL, PANEL))],
        out_specs=(pl.BlockSpec((PANEL, 2 * PANEL), lambda i: (i, 0)),) * 2,
        scratch_shapes=buffers,
        compiler_params=LIMIT,
        cost_estimate=pl.CostEstimate(flops=10**10, bytes_accessed=10 * 2**20, transcendentals=0),
        name="strip",
    )(place, row_owner, col_owner, strip_tiles, inverse, corner_h)

    factor, left_high, left_low = pl.pallas_call(
        band_kernel,
        grid=(band // PANEL,),
        out_shape=(shape_of((band, PANEL)),) + (shape_of((band, 2 * PANEL), BF16),) * 2,
        in_specs=[SMEM, SMEM, SMEM, whole(band_tiles.shape), whole((PANEL, PANEL))],
        out_specs=(pl.BlockSpec((PANEL, PANEL), lambda i: (i, 0)),)
        + (pl.BlockSpec((PANEL, 2 * PANEL), lambda i: (i, 0)),) * 2,
        scratch_shapes=buffers,
        compiler_params=LIMIT,
        cost_estimate=pl.CostEstimate(flops=13 * 10**9, bytes_accessed=20 * 2**20, transcendentals=0),
        name="band",
    )(place, row_owner, col_owner, band_tiles, inverse)

    tall = 256
    h_block = pl.pallas_call(
        final_kernel,
        grid=(band // tall,),
        out_shape=shape_of((band, strip)),
        in_specs=[SMEM, SMEM, SMEM, whole(h_tiles.shape)]
        + [pl.BlockSpec((tall, 2 * PANEL), lambda i: (i, 0))] * 2
        + [whole((strip, 2 * PANEL))] * 2,
        out_specs=pl.BlockSpec((tall, strip), lambda i: (i, 0)),
        compiler_params=LIMIT,
        cost_estimate=pl.CostEstimate(flops=13 * 10**9, bytes_accessed=28 * 2**20, transcendentals=0),
        name="final",
    )(place, row_owner, col_owner, h_tiles, left_high, left_low, right_high, right_low)
    return h_block, factor


def solution(mesh):
    in_specs = (P("row", "col", None, None), P("row", "col", None, None), P(), P())
    out_specs = (P("row", "col"), P("row", None))
    return jax.shard_map(
        per_device, mesh=mesh, in_specs=in_specs, out_specs=out_specs, check_vma=False
    )
```

```python
import jax
import jax.numpy as jnp
from jax import lax
from jax.experimental import pallas as pl
from jax.experimental.pallas import tpu as pltpu
from jax.sharding import PartitionSpec as P

ORDER = 16384
PANEL = 512
BLOCK = 64
STEP = 128
HIGHEST = lax.Precision.HIGHEST
BF16 = jnp.bfloat16
F32 = jnp.float32


def dot(a, b, ca, cb, precision=None):
    return lax.dot_general(
        a, b, (((ca,), (cb,)), ((), ())), precision=precision, preferred_element_type=F32
    )


def halves(x):
    high = x.astype(BF16)
    return high, (x - high.astype(F32)).astype(BF16)


def lower_half(shape):
    return lax.broadcasted_iota(jnp.int32, shape, 1) < BLOCK


def fetch_panel(read, rows, first, row_owner, col_owner, s_out, h_out):
    low = lower_half((BLOCK, 2 * BLOCK))
    for i in range(rows):
        p = row_owner[first + i]
        for k in range(0, PANEL // BLOCK, 2):
            one = read(i, p, col_owner[k])
            two = read(i, p, col_owner[k + 1])
            at = (pl.ds(i * BLOCK, BLOCK), pl.ds(k * BLOCK, 2 * BLOCK))
            s_out[at] = jnp.where(low, one, pltpu.roll(two, BLOCK, 1))
            h_out[at] = jnp.where(low, pltpu.roll(one, BLOCK, 1), two)


def spread(x, rows):
    return jnp.broadcast_to(x, (rows, x.shape[1]))


def factor_inverse(a_ref, b_ref):
    sub = lax.broadcasted_iota(jnp.int32, (8, STEP), 0)
    for j in range(0, STEP, 8):
        far = STEP - j - 8
        a_near, b_near = a_ref[j : j + 8, :], b_ref[j : j + 8, :]
        near = [jnp.broadcast_to(a_near[:, j + t : j + t + 1], (8, STEP)) for t in range(8)]
        if far:
            a_far, b_far = a_ref[j + 8 :, :], b_ref[j + 8 :, :]
            cols = [jnp.broadcast_to(a_far[:, j + t : j + t + 1], (far, STEP)) for t in range(8)]
        scales, links = [], []
        for t in range(8):
            r = lax.rsqrt(near[t][t : t + 1, :])
            l = near[t] * spread(r, 8)
            below = jnp.where(sub > t, l, 0.0)
            a_row, b_row = a_near[t : t + 1, :] * r, b_near[t : t + 1, :] * r
            a_near = jnp.where(sub == t, spread(a_row, 8), a_near - below * spread(a_row, 8))
            b_near = jnp.where(sub == t, spread(b_row, 8), b_near - below * spread(b_row, 8))
            link = {}
            for u in range(t + 1, 8):
                link[u] = l[u : u + 1, :]
                near[u] = near[u] - l * spread(link[u], 8)
            scales.append(r)
            links.append(link)
        b_ref[j : j + 8, :] = b_near
        if far:
            for t in range(8):
                l = cols[t] * spread(scales[t], far)
                for u in range(t + 1, 8):
                    cols[u] = cols[u] - l * spread(links[t][u], far)
                a_far = a_far - l * spread(a_near[t : t + 1, :], far)
                b_far = b_far - l * spread(b_near[t : t + 1, :], far)
            a_ref[j + 8 :, :] = a_far
            b_ref[j + 8 :, :] = b_far


def corner_kernel(row_owner, col_owner, tiles, inverse, corner_h, s_top, work, a_blk, b_blk):
    fetch_panel(
        lambda i, p, q: tiles[2 * q + p % 2, p // 2, 2],
        PANEL // BLOCK, 0, row_owner, col_owner, s_top, corner_h,
    )
    eye = lax.broadcasted_iota(jnp.int32, (STEP, STEP), 0) == lax.broadcasted_iota(
        jnp.int32, (STEP, STEP), 1
    )
    eye = jnp.where(eye, 1.0, 0.0)
    count = PANEL // STEP
    for k in range(count):
        work[k, :, :PANEL] = s_top[k * STEP : (k + 1) * STEP, :]
        work[k, :, PANEL:] = jnp.zeros((STEP, PANEL), F32)
        work[k, :, PANEL + k * STEP : PANEL + (k + 1) * STEP] = eye
    lane = lax.broadcasted_iota(jnp.int32, (STEP, PANEL), 1)

    def step(k, carry):
        a_blk[...] = work[k, :, pl.ds(pl.multiple_of(k * STEP, STEP), STEP)]
        b_blk[...] = eye
        factor_inverse(a_blk, b_blk)
        rows = dot(b_blk[...], work[k], 1, 0, HIGHEST)
        work[k] = rows
        ahead = jnp.where(lane >= (k + 1) * STEP, rows[:, :PANEL], 0.0).T
        for i in range(1, count):
            work[i] = work[i] - dot(ahead[i * STEP : (i + 1) * STEP], rows, 1, 0, HIGHEST)
        return carry

    lax.fori_loop(0, count, step, 0)
    for k in range(count):
        inverse[k * STEP : (k + 1) * STEP, :] = work[k, :, PANEL:]


def coupling_of(s_rows, inverse, special):
    factor = dot(s_rows, inverse, 1, 1, HIGHEST)
    coupling = dot(factor, inverse, 1, 0, HIGHEST)
    shape = (PANEL, PANEL)
    eye = lax.broadcasted_iota(jnp.int32, shape, 0) == lax.broadcasted_iota(jnp.int32, shape, 1)
    return factor, jnp.where(special, jnp.where(eye, 1.0, 0.0) - inverse, coupling)


def strip_kernel(place, row_owner, col_owner, tiles, inv, corner_h, high, low, s_buf, h_buf):
    step = pl.program_id(0)
    here = place[1]
    fetch_panel(
        lambda i, p, q: tiles[p // 2, 2 * q + p % 2],
        PANEL // BLOCK, here * 16 + step * 8, row_owner, col_owner, s_buf, h_buf,
    )
    special = jnp.logical_and(here == 0, step == 0)
    _, coupling = coupling_of(s_buf[...], inv[...], special)
    rest = h_buf[...] - dot(coupling, corner_h[...], 1, 0, HIGHEST)
    high[:, :PANEL], low[:, :PANEL] = halves(rest)
    high[:, PANEL:], low[:, PANEL:] = halves(coupling)


def band_kernel(place, row_owner, col_owner, tiles, inv, factor, high, low, s_buf, h_buf):
    step = pl.program_id(0)
    here = place[0]
    slot = step // 2
    fetch_panel(
        lambda i, p, q: tiles[2 * q + p % 2, p // 2, slot],
        PANEL // BLOCK, here * 32 + step * 8, row_owner, col_owner, s_buf, h_buf,
    )
    special = jnp.logical_and(here == 0, step == 0)
    factor[...], coupling = coupling_of(s_buf[...], inv[...], special)
    high[:, :PANEL], low[:, :PANEL] = halves(coupling)
    high[:, PANEL:], low[:, PANEL:] = halves(h_buf[...])


def final_kernel(place, row_owner, col_owner, tiles, lh, ll, rh, rl, out):
    step = pl.program_id(0)
    blocks = out.shape[0] // BLOCK
    update = dot(lh[...], rh[...], 1, 1)
    update = update + dot(lh[...], rl[...], 1, 1)
    update = update + dot(ll[...], rh[...], 1, 1)
    out[...] = update
    low = lower_half((BLOCK, 2 * BLOCK))
    slot = pl.multiple_of(step * blocks // 16 * BLOCK, BLOCK)
    for i in range(blocks):
        p = row_owner[place[0] * 32 + step * blocks + i]
        for j in range(0, 16, 2):
            one = tiles[p // 2, 2 * col_owner[place[1] * 16 + j] + p % 2, pl.ds(slot, BLOCK), :]
            two = tiles[p // 2, 2 * col_owner[place[1] * 16 + j + 1] + p % 2, pl.ds(slot, BLOCK), :]
            if j < 8:
                both = jnp.where(low, one, pltpu.roll(two, BLOCK, 1))
            else:
                both = jnp.where(low, pltpu.roll(one, BLOCK, 1), two)
            at = (pl.ds(i * BLOCK, BLOCK), pl.ds(j * BLOCK, 2 * BLOCK))
            out[at] = both - out[at]


def axis_split(r, c):
    return r // 2, r % 2, c // 8, (c // 2) % 4, c % 2


def exchange_kernel(panels, h_ref, zs, xs, outgoing, h_buf, load_sem, store_sem, own_sem,
                    p1s, p1z, p1t, p1x, sends, gets, sib_s, sib_r):
    r, c = lax.axis_index("row"), lax.axis_index("col")
    x, yl, yh, z, core = axis_split(r, c)
    half_r, half_c = zs.shape[1] // 2, xs.shape[1] // 2

    def col_of(yh_, z_, core_):
        return yh_ * 8 + (z_ % 4) * 2 + core_

    def row_of(x_, yl_):
        return (x_ % 4) * 2 + yl_

    barrier = pltpu.get_barrier_semaphore()
    for d in range(1, 8):
        pl.semaphore_signal(barrier, inc=1, device_id=((r + d) % 8, c), device_id_type=pl.DeviceIdType.MESH)
    for d in range(1, 16):
        pl.semaphore_signal(barrier, inc=1, device_id=(r, (c + d) % 16), device_id_type=pl.DeviceIdType.MESH)
    loads = []
    for i in range(8):
        rows = pl.ds(i * 128, 128)
        loads.append(pltpu.make_async_copy(h_ref.at[rows], h_buf.at[rows], load_sem.at[i]))
        loads[-1].start()
    pl.semaphore_wait(barrier, 22)

    def send(src, dst, ss, rs, to):
        copy = pltpu.make_async_remote_copy(
            src_ref=src, dst_ref=dst, send_sem=ss, recv_sem=rs, device_id=to,
            device_id_type=pl.DeviceIdType.MESH,
        )
        copy.start()
        return copy

    def arrived(ref, sem):
        pltpu.make_async_copy(ref, ref, sem).wait()

    open_sends = []
    for d in range(1, 8):
        to = (r + d) % 8
        open_sends.append(send(panels.at[0], zs.at[c, r, 2], p1s.at[0, d], p1z.at[d], (to, c)))
        open_sends.append(
            send(panels.at[pl.ds(2 * to, 2)], zs.at[c, r, pl.ds(0, 2)], p1s.at[1, d], p1z.at[d], (to, c))
        )
    for d in range(1, 16):
        to = (c + d) % 16
        open_sends.append(send(panels.at[to], xs.at[r, c], p1t.at[d], p1x.at[d], (r, to)))
    own = [
        pltpu.make_async_copy(panels.at[0], zs.at[c, r, 2], own_sem.at[0]),
        pltpu.make_async_copy(panels.at[pl.ds(2 * r, 2)], zs.at[c, r, pl.ds(0, 2)], own_sem.at[1]),
        pltpu.make_async_copy(panels.at[c], xs.at[r, c], own_sem.at[2]),
    ]
    for copy in own:
        copy.start()

    zp, zm = (r, col_of(yh, z + 1, core)), (r, col_of(yh, z + 3, core))
    yp, sib = (r, col_of(1 - yh, z, core)), (r, col_of(yh, z, 1 - core))
    xp, xm, lp = (row_of(x + 1, yl), c), (row_of(x + 3, yl), c), (row_of(x, 1 - yl), c)

    def chunk_z(k):
        return zs.at[k]

    def chunk_x(k):
        return xs.at[k]

    def first(ref, k):
        return ref.at[k, pl.ds(0, ref.shape[1] // 2)]

    def second(ref, k):
        return ref.at[k, pl.ds(ref.shape[1] // 2, ref.shape[1] // 2)]

    def out(ref, i, to):
        open_sends.append(send(ref, ref, sends.at[i], gets.at[i], to))

    def share(k, i):
        open_sends.append(send(zs.at[k], zs.at[k], sib_s.at[i], sib_r.at[i], sib))

    own[0].wait()
    own[1].wait()
    for d in range(1, 8):
        arrived(zs.at[c, (r + 8 - d) % 8], p1z.at[d])
    out(chunk_z(c), 0, yp)
    out(chunk_z(c), 1, zp)
    out(chunk_z(c), 2, zm)
    own[2].wait()
    for d in range(1, 16):
        arrived(xs.at[r, (c + 16 - d) % 16], p1x.at[d])
    out(chunk_x(r), 3, lp)
    out(chunk_x(r), 4, xp)
    out(chunk_x(r), 5, xm)
    share(c, 0)

    for i in range(8):
        loads[i].wait()

    def tile(n, carry):
        i, j = n // 16, n % 16
        columns = pl.ds(pl.multiple_of(j * 128, 128), 128)
        rows = pl.ds(pl.multiple_of(i * 128, 128), 128)
        pltpu.make_async_copy(h_buf.at[rows, columns], outgoing.at[i, j], store_sem).start()
        return carry

    lax.fori_loop(0, 128, tile, 0)

    def c_at(yh_, dz):
        return col_of(yh_, z + dz, core)

    arrived(chunk_x(row_of(x + 3, yl)), gets.at[4])
    out(first(xs, row_of(x + 3, yl)), 6, xp)
    arrived(chunk_x(row_of(x + 1, yl)), gets.at[5])
    out(second(xs, row_of(x + 1, yl)), 7, xm)
    arrived(chunk_x(row_of(x, 1 - yl)), gets.at[3])
    out(chunk_x(row_of(x, 1 - yl)), 8, xp)
    out(chunk_x(row_of(x, 1 - yl)), 9, xm)

    arrived(chunk_z(c_at(yh, 3)), gets.at[1])
    out(first(zs, c_at(yh, 3)), 10, zp)
    arrived(chunk_z(c_at(yh, 1)), gets.at[2])
    out(second(zs, c_at(yh, 1)), 11, zm)
    arrived(chunk_z(c_at(1 - yh, 0)), gets.at[0])
    out(chunk_z(c_at(1 - yh, 0)), 12, zp)
    out(chunk_z(c_at(1 - yh, 0)), 13, zm)
    share(c_at(yh, 3), 1)
    share(c_at(yh, 1), 2)
    share(c_at(1 - yh, 0), 3)

    arrived(chunk_x(row_of(x + 3, 1 - yl)), gets.at[8])
    out(first(xs, row_of(x + 3, 1 - yl)), 14, xp)
    arrived(chunk_x(row_of(x + 1, 1 - yl)), gets.at[9])
    out(second(xs, row_of(x + 1, 1 - yl)), 15, xm)

    arrived(first(zs, c_at(yh, 2)), gets.at[10])
    arrived(second(zs, c_at(yh, 2)), gets.at[11])
    share(c_at(yh, 2), 4)
    arrived(chunk_z(c_at(1 - yh, 3)), gets.at[12])
    out(first(zs, c_at(1 - yh, 3)), 16, zp)
    arrived(chunk_z(c_at(1 - yh, 1)), gets.at[13])
    out(second(zs, c_at(1 - yh, 1)), 17, zm)
    share(c_at(1 - yh, 3), 5)
    share(c_at(1 - yh, 1), 6)

    arrived(first(xs, row_of(x + 2, yl)), gets.at[6])
    arrived(second(xs, row_of(x + 2, yl)), gets.at[7])
    arrived(first(xs, row_of(x + 2, 1 - yl)), gets.at[14])
    arrived(second(xs, row_of(x + 2, 1 - yl)), gets.at[15])
    arrived(first(zs, c_at(1 - yh, 2)), gets.at[16])
    arrived(second(zs, c_at(1 - yh, 2)), gets.at[17])
    share(c_at(1 - yh, 2), 7)

    def theirs(yh_, dz):
        return zs.at[col_of(yh_, z + dz, 1 - core)]

    order = [(yh, 0), (yh, 3), (yh, 1), (1 - yh, 0), (yh, 2), (1 - yh, 3), (1 - yh, 1), (1 - yh, 2)]
    for i, (yh_, dz) in enumerate(order):
        arrived(theirs(yh_, dz), sib_r.at[i])
    arrived(outgoing, store_sem)
    for copy in open_sends:
        copy.wait_send()


def exchange(panels, local_h):
    any_space = pl.BlockSpec(memory_space=pl.ANY)
    dma = pltpu.SemaphoreType.DMA
    return pl.pallas_call(
        exchange_kernel,
        out_shape=(
            shape_of((16, 8, 3, BLOCK, 128)),
            shape_of((8, 16, BLOCK, 128)),
            shape_of((8, 16, 128, 128)),
        ),
        in_specs=[pl.BlockSpec(memory_space=pltpu.VMEM), any_space],
        out_specs=(any_space,) * 3,
        scratch_shapes=[
            pltpu.VMEM(local_h.shape, F32), dma((8,)), dma, dma((3,)),
            dma((2, 8)), dma((8,)), dma((16,)), dma((16,)), dma((18,)), dma((18,)), dma((8,)), dma((8,)),
        ],
        compiler_params=pltpu.CompilerParams(
            collective_id=0, has_side_effects=True, vmem_limit_bytes=60 * 2**20
        ),
        cost_estimate=pl.CostEstimate(flops=0, bytes_accessed=64 * 2**20, transcendentals=0),
        name="exchange",
    )(panels, local_h)


def whole(shape):
    return pl.BlockSpec(shape, lambda *i: (0,) * len(shape), pipeline_mode=pl.Buffered(1))


SMEM = pl.BlockSpec(memory_space=pltpu.SMEM)
LIMIT = pltpu.CompilerParams(vmem_limit_bytes=60 * 2**20)


def shape_of(shape, dtype=F32):
    return jax.ShapeDtypeStruct(shape, dtype)


def per_device(h_old, s_old, row_owner, col_owner):
    rows_n = lax.axis_size("row")
    cols_n = lax.axis_size("col")
    row_id = lax.axis_index("row")
    col_id = lax.axis_index("col")
    place = jnp.stack([row_id, col_id]).astype(jnp.int32)
    local_h = h_old[0, 0]
    local_s = s_old[0, 0]
    band = ORDER // rows_n
    strip = ORDER // cols_n
    panels = jnp.concatenate([local_s, local_h[:, :BLOCK]], axis=1)
    band_tiles, strip_tiles, outgoing = exchange(panels.reshape(16, BLOCK, 128), local_h)
    h_tiles = lax.all_to_all(
        outgoing.reshape(rows_n * cols_n, 128, 128), ("row", "col"), 0, 0, tiled=True
    ).reshape(rows_n, cols_n, 128, 128)

    inverse, corner_h = pl.pallas_call(
        corner_kernel,
        out_shape=(shape_of((PANEL, PANEL)), shape_of((PANEL, PANEL))),
        in_specs=[SMEM, SMEM, pl.BlockSpec(memory_space=pltpu.VMEM)],
        scratch_shapes=[
            pltpu.VMEM((PANEL, PANEL), F32),
            pltpu.VMEM((PANEL // STEP, STEP, 2 * PANEL), F32),
            pltpu.VMEM((STEP, STEP), F32),
            pltpu.VMEM((STEP, STEP), F32),
        ],
        compiler_params=LIMIT,
        cost_estimate=pl.CostEstimate(flops=3 * 10**10, bytes_accessed=6 * 2**20, transcendentals=0),
        name="corner",
    )(row_owner, col_owner, band_tiles)

    buffers = [pltpu.VMEM((PANEL, PANEL), F32), pltpu.VMEM((PANEL, PANEL), F32)]
    right_high, right_low = pl.pallas_call(
        strip_kernel,
        grid=(strip // PANEL,),
        out_shape=(shape_of((strip, 2 * PANEL), BF16),) * 2,
        in_specs=[SMEM, SMEM, SMEM, whole(strip_tiles.shape), whole((PANEL, PANEL)), whole((PANEL, PANEL))],
        out_specs=(pl.BlockSpec((PANEL, 2 * PANEL), lambda i: (i, 0)),) * 2,
        scratch_shapes=buffers,
        compiler_params=LIMIT,
        cost_estimate=pl.CostEstimate(flops=10**10, bytes_accessed=10 * 2**20, transcendentals=0),
        name="strip",
    )(place, row_owner, col_owner, strip_tiles, inverse, corner_h)

    factor, left_high, left_low = pl.pallas_call(
        band_kernel,
        grid=(band // PANEL,),
        out_shape=(shape_of((band, PANEL)),) + (shape_of((band, 2 * PANEL), BF16),) * 2,
        in_specs=[SMEM, SMEM, SMEM, whole(band_tiles.shape), whole((PANEL, PANEL))],
        out_specs=(pl.BlockSpec((PANEL, PANEL), lambda i: (i, 0)),)
        + (pl.BlockSpec((PANEL, 2 * PANEL), lambda i: (i, 0)),) * 2,
        scratch_shapes=buffers,
        compiler_params=LIMIT,
        cost_estimate=pl.CostEstimate(flops=13 * 10**9, bytes_accessed=20 * 2**20, transcendentals=0),
        name="band",
    )(place, row_owner, col_owner, band_tiles, inverse)

    tall = 256
    h_block = pl.pallas_call(
        final_kernel,
        grid=(band // tall,),
        out_shape=shape_of((band, strip)),
        in_specs=[SMEM, SMEM, SMEM, whole(h_tiles.shape)]
        + [pl.BlockSpec((tall, 2 * PANEL), lambda i: (i, 0))] * 2
        + [whole((strip, 2 * PANEL))] * 2,
        out_specs=pl.BlockSpec((tall, strip), lambda i: (i, 0)),
        compiler_params=LIMIT,
        cost_estimate=pl.CostEstimate(flops=13 * 10**9, bytes_accessed=28 * 2**20, transcendentals=0),
        name="final",
    )(place, row_owner, col_owner, h_tiles, left_high, left_low, right_high, right_low)
    return h_block, factor


def solution(mesh):
    in_specs = (P("row", "col", None, None), P("row", "col", None, None), P(), P())
    out_specs = (P("row", "col"), P("row", None))
    return jax.shard_map(
        per_device, mesh=mesh, in_specs=in_specs, out_specs=out_specs, check_vma=False
    )
```

```python
import functools

import jax
import jax.numpy as jnp
from jax import lax
from jax.experimental import pallas as pl
from jax.experimental.pallas import tpu as pltpu
from jax.sharding import PartitionSpec as P

ORDER = 16384
PANEL = 512
BLOCK = 64
STEP = 128
HIGHEST = lax.Precision.HIGHEST
BF16 = jnp.bfloat16
F32 = jnp.float32


def dot(a, b, ca, cb, precision=None):
    return lax.dot_general(
        a, b, (((ca,), (cb,)), ((), ())), precision=precision, preferred_element_type=F32
    )


def halves(x):
    high = x.astype(BF16)
    return high, (x - high.astype(F32)).astype(BF16)


def lower_half(shape):
    return lax.broadcasted_iota(jnp.int32, shape, 1) < BLOCK


def fetch_panel(read, rows, first, row_owner, col_owner, s_out, h_out):
    low = lower_half((BLOCK, 2 * BLOCK))
    for i in range(rows):
        p = row_owner[first + i]
        for k in range(0, PANEL // BLOCK, 2):
            one = read(i, p, col_owner[k])
            two = read(i, p, col_owner[k + 1])
            at = (pl.ds(i * BLOCK, BLOCK), pl.ds(k * BLOCK, 2 * BLOCK))
            s_out[at] = jnp.where(low, one, pltpu.roll(two, BLOCK, 1))
            h_out[at] = jnp.where(low, pltpu.roll(one, BLOCK, 1), two)


def spread(x, rows):
    return jnp.broadcast_to(x, (rows, x.shape[1]))


def factor_inverse(a_ref, b_ref):
    sub = lax.broadcasted_iota(jnp.int32, (8, STEP), 0)
    for j in range(0, STEP, 8):
        far = STEP - j - 8
        a_near, b_near = a_ref[j : j + 8, :], b_ref[j : j + 8, :]
        near = [jnp.broadcast_to(a_near[:, j + t : j + t + 1], (8, STEP)) for t in range(8)]
        if far:
            a_far, b_far = a_ref[j + 8 :, :], b_ref[j + 8 :, :]
            cols = [jnp.broadcast_to(a_far[:, j + t : j + t + 1], (far, STEP)) for t in range(8)]
        scales, links = [], []
        for t in range(8):
            r = lax.rsqrt(near[t][t : t + 1, :])
            l = near[t] * spread(r, 8)
            below = jnp.where(sub > t, l, 0.0)
            a_row, b_row = a_near[t : t + 1, :] * r, b_near[t : t + 1, :] * r
            a_near = jnp.where(sub == t, spread(a_row, 8), a_near - below * spread(a_row, 8))
            b_near = jnp.where(sub == t, spread(b_row, 8), b_near - below * spread(b_row, 8))
            link = {}
            for u in range(t + 1, 8):
                link[u] = l[u : u + 1, :]
                near[u] = near[u] - l * spread(link[u], 8)
            scales.append(r)
            links.append(link)
        b_ref[j : j + 8, :] = b_near
        if far:
            for t in range(8):
                l = cols[t] * spread(scales[t], far)
                for u in range(t + 1, 8):
                    cols[u] = cols[u] - l * spread(links[t][u], far)
                a_far = a_far - l * spread(a_near[t : t + 1, :], far)
                b_far = b_far - l * spread(b_near[t : t + 1, :], far)
            a_ref[j + 8 :, :] = a_far
            b_ref[j + 8 :, :] = b_far


def corner_kernel(row_owner, col_owner, tiles, inverse, corner_h, s_top, work, a_blk, b_blk):
    fetch_panel(
        lambda i, p, q: tiles[2 * q + p % 2, p // 2, 0],
        PANEL // BLOCK, 0, row_owner, col_owner, s_top, corner_h,
    )
    eye = lax.broadcasted_iota(jnp.int32, (STEP, STEP), 0) == lax.broadcasted_iota(
        jnp.int32, (STEP, STEP), 1
    )
    eye = jnp.where(eye, 1.0, 0.0)
    count = PANEL // STEP
    for k in range(count):
        work[k, :, :PANEL] = s_top[k * STEP : (k + 1) * STEP, :]
        work[k, :, PANEL:] = jnp.zeros((STEP, PANEL), F32)
        work[k, :, PANEL + k * STEP : PANEL + (k + 1) * STEP] = eye
    lane = lax.broadcasted_iota(jnp.int32, (STEP, PANEL), 1)

    def step(k, carry):
        a_blk[...] = work[k, :, pl.ds(pl.multiple_of(k * STEP, STEP), STEP)]
        b_blk[...] = eye
        factor_inverse(a_blk, b_blk)
        rows = dot(b_blk[...], work[k], 1, 0, HIGHEST)
        work[k] = rows
        ahead = jnp.where(lane >= (k + 1) * STEP, rows[:, :PANEL], 0.0).T
        for i in range(1, count):
            work[i] = work[i] - dot(ahead[i * STEP : (i + 1) * STEP], rows, 1, 0, HIGHEST)
        return carry

    lax.fori_loop(0, count, step, 0)
    for k in range(count):
        inverse[k * STEP : (k + 1) * STEP, :] = work[k, :, PANEL:]


def coupling_of(s_rows, inverse, special):
    factor = dot(s_rows, inverse, 1, 1, HIGHEST)
    coupling = dot(factor, inverse, 1, 0, HIGHEST)
    shape = (PANEL, PANEL)
    eye = lax.broadcasted_iota(jnp.int32, shape, 0) == lax.broadcasted_iota(jnp.int32, shape, 1)
    return factor, jnp.where(special, jnp.where(eye, 1.0, 0.0) - inverse, coupling)


def strip_kernel(place, row_owner, col_owner, tiles, inv, corner_h, high, low, s_buf, h_buf):
    step = pl.program_id(0)
    here = place[1]
    fetch_panel(
        lambda i, p, q: tiles[p // 2, 2 * q + p % 2],
        PANEL // BLOCK, here * 16 + step * 8, row_owner, col_owner, s_buf, h_buf,
    )
    special = jnp.logical_and(here == 0, step == 0)
    _, coupling = coupling_of(s_buf[...], inv[...], special)
    rest = h_buf[...] - dot(coupling, corner_h[...], 1, 0, HIGHEST)
    high[:, :PANEL], low[:, :PANEL] = halves(rest)
    high[:, PANEL:], low[:, PANEL:] = halves(coupling)


def band_kernel(place, row_owner, col_owner, tiles, inv, factor, high, low, s_buf, h_buf):
    step = pl.program_id(0)
    here = place[0]
    fetch_panel(
        lambda i, p, q: tiles[2 * q + p % 2, p // 2, 0],
        PANEL // BLOCK, here * 32 + step * 8, row_owner, col_owner, s_buf, h_buf,
    )
    special = jnp.logical_and(here == 0, step == 0)
    factor[...], coupling = coupling_of(s_buf[...], inv[...], special)
    high[:, :PANEL], low[:, :PANEL] = halves(coupling)
    high[:, PANEL:], low[:, PANEL:] = halves(h_buf[...])


def final_kernel(part, place, row_owner, col_owner, tiles, lh, ll, rh, rl, *refs):
    out = refs[-1]
    step = pl.program_id(0)
    blocks = out.shape[0] // BLOCK
    update = dot(lh[...], rh[...], 1, 1)
    update = update + dot(lh[...], rl[...], 1, 1)
    update = update + dot(ll[...], rh[...], 1, 1)
    out[...] = update
    low = lower_half((BLOCK, 2 * BLOCK))
    for i in range(blocks):
        p = row_owner[place[0] * 32 + part * 16 + step * blocks + i]
        for j in range(0, 16, 2):
            one = tiles[p // 2, 2 * col_owner[place[1] * 16 + j] + p % 2]
            two = tiles[p // 2, 2 * col_owner[place[1] * 16 + j + 1] + p % 2]
            if j < 8:
                both = jnp.where(low, one, pltpu.roll(two, BLOCK, 1))
            else:
                both = jnp.where(low, pltpu.roll(one, BLOCK, 1), two)
            at = (pl.ds(i * BLOCK, BLOCK), pl.ds(j * BLOCK, 2 * BLOCK))
            out[at] = both - out[at]


def axis_split(r, c):
    return r // 2, r % 2, c // 8, (c // 2) % 4, c % 2


def exchange_kernel(panels, h_ref, zs, xs, near, outgoing, h_buf, load_sem, store_sem, own_sem,
                    p1s, p1z, p1t, p1x, sends, gets, sib_s, sib_r, h_sent, h_got):
    r, c = lax.axis_index("row"), lax.axis_index("col")
    x, yl, yh, z, core = axis_split(r, c)
    half_r, half_c = zs.shape[1] // 2, xs.shape[1] // 2

    def col_of(yh_, z_, core_):
        return yh_ * 8 + (z_ % 4) * 2 + core_

    def row_of(x_, yl_):
        return (x_ % 4) * 2 + yl_

    loads = []
    for i in range(8):
        rows = pl.ds(i * 128, 128)
        loads.append(pltpu.make_async_copy(h_ref.at[rows], h_buf.at[rows], load_sem.at[i]))
        loads[-1].start()

    def send(src, dst, ss, rs, to):
        copy = pltpu.make_async_remote_copy(
            src_ref=src, dst_ref=dst, send_sem=ss, recv_sem=rs, device_id=to,
            device_id_type=pl.DeviceIdType.MESH,
        )
        copy.start()
        return copy

    def arrived(ref, sem):
        pltpu.make_async_copy(ref, ref, sem).wait()

    open_sends = []
    for d in range(1, 8):
        to = (r + d) % 8
        open_sends.append(send(panels.at[0], zs.at[c, r, 2], p1s.at[0, d], p1z.at[d], (to, c)))
        open_sends.append(
            send(panels.at[pl.ds(2 * to, 2)], zs.at[c, r, pl.ds(0, 2)], p1s.at[1, d], p1z.at[d], (to, c))
        )
    for d in range(1, 16):
        to = (c + d) % 16
        open_sends.append(send(panels.at[to], xs.at[r, c], p1t.at[d], p1x.at[d], (r, to)))
    own = [
        pltpu.make_async_copy(panels.at[0], zs.at[c, r, 2], own_sem.at[0]),
        pltpu.make_async_copy(panels.at[pl.ds(2 * r, 2)], zs.at[c, r, pl.ds(0, 2)], own_sem.at[1]),
        pltpu.make_async_copy(panels.at[c], xs.at[r, c], own_sem.at[2]),
    ]
    for copy in own:
        copy.start()

    for i in range(8):
        loads[i].wait()

    def upper(i, j):
        rows = pl.ds(pl.multiple_of(i * 128, 128), BLOCK)
        return h_buf.at[rows, pl.ds(pl.multiple_of(j * 128, 128), 128)]

    def send_tile(n, carry):
        i, j = (r + n % 8) % 8, (c + n // 8) % 16
        pltpu.make_async_remote_copy(
            src_ref=upper(i, j), dst_ref=near.at[r * 16 + c], send_sem=h_sent, recv_sem=h_got,
            device_id=(i, j), device_id_type=pl.DeviceIdType.MESH,
        ).start()
        return carry

    def batch(n):
        lax.fori_loop(max(16 * n, 1), 16 * n + 16, send_tile, 0)

    def store_tile(n, carry):
        i, j = n // 16, n % 16
        rows = pl.ds(pl.multiple_of(i * 128 + BLOCK, BLOCK), BLOCK)
        columns = pl.ds(pl.multiple_of(j * 128, 128), 128)
        pltpu.make_async_copy(h_buf.at[rows, columns], outgoing.at[i, j], store_sem).start()
        return carry

    batch(0)
    pltpu.make_async_copy(upper(r, c), near.at[r * 16 + c], h_got).start()

    zp, zm = (r, col_of(yh, z + 1, core)), (r, col_of(yh, z + 3, core))
    yp, sib = (r, col_of(1 - yh, z, core)), (r, col_of(yh, z, 1 - core))
    xp, xm, lp = (row_of(x + 1, yl), c), (row_of(x + 3, yl), c), (row_of(x, 1 - yl), c)

    def chunk_z(k):
        return zs.at[k]

    def chunk_x(k):
        return xs.at[k]

    def first(ref, k):
        return ref.at[k, pl.ds(0, ref.shape[1] // 2)]

    def second(ref, k):
        return ref.at[k, pl.ds(ref.shape[1] // 2, ref.shape[1] // 2)]

    def out(ref, i, to):
        open_sends.append(send(ref, ref, sends.at[i], gets.at[i], to))

    def share(k, i):
        open_sends.append(send(zs.at[k], zs.at[k], sib_s.at[i], sib_r.at[i], sib))

    own[0].wait()
    own[1].wait()
    for d in range(1, 8):
        arrived(zs.at[c, (r + 8 - d) % 8], p1z.at[d])
    out(chunk_z(c), 0, yp)
    out(chunk_z(c), 1, zp)
    out(chunk_z(c), 2, zm)
    own[2].wait()
    for d in range(1, 16):
        arrived(xs.at[r, (c + 16 - d) % 16], p1x.at[d])
    out(chunk_x(r), 3, lp)
    out(chunk_x(r), 4, xp)
    out(chunk_x(r), 5, xm)
    share(c, 0)
    lax.fori_loop(0, 128, store_tile, 0)
    batch(1)

    def c_at(yh_, dz):
        return col_of(yh_, z + dz, core)

    arrived(chunk_x(row_of(x + 3, yl)), gets.at[4])
    out(first(xs, row_of(x + 3, yl)), 6, xp)
    arrived(chunk_x(row_of(x + 1, yl)), gets.at[5])
    out(second(xs, row_of(x + 1, yl)), 7, xm)
    batch(2)
    arrived(chunk_x(row_of(x, 1 - yl)), gets.at[3])
    out(chunk_x(row_of(x, 1 - yl)), 8, xp)
    out(chunk_x(row_of(x, 1 - yl)), 9, xm)
    batch(3)

    arrived(chunk_z(c_at(yh, 3)), gets.at[1])
    out(first(zs, c_at(yh, 3)), 10, zp)
    arrived(chunk_z(c_at(yh, 1)), gets.at[2])
    out(second(zs, c_at(yh, 1)), 11, zm)
    batch(4)
    arrived(chunk_z(c_at(1 - yh, 0)), gets.at[0])
    out(chunk_z(c_at(1 - yh, 0)), 12, zp)
    out(chunk_z(c_at(1 - yh, 0)), 13, zm)
    batch(5)
    share(c_at(yh, 3), 1)
    share(c_at(yh, 1), 2)
    share(c_at(1 - yh, 0), 3)

    arrived(chunk_x(row_of(x + 3, 1 - yl)), gets.at[8])
    out(first(xs, row_of(x + 3, 1 - yl)), 14, xp)
    arrived(chunk_x(row_of(x + 1, 1 - yl)), gets.at[9])
    out(second(xs, row_of(x + 1, 1 - yl)), 15, xm)
    batch(6)

    arrived(first(zs, c_at(yh, 2)), gets.at[10])
    arrived(second(zs, c_at(yh, 2)), gets.at[11])
    share(c_at(yh, 2), 4)
    arrived(chunk_z(c_at(1 - yh, 3)), gets.at[12])
    out(first(zs, c_at(1 - yh, 3)), 16, zp)
    arrived(chunk_z(c_at(1 - yh, 1)), gets.at[13])
    out(second(zs, c_at(1 - yh, 1)), 17, zm)
    batch(7)
    share(c_at(1 - yh, 3), 5)
    share(c_at(1 - yh, 1), 6)

    arrived(first(xs, row_of(x + 2, yl)), gets.at[6])
    arrived(second(xs, row_of(x + 2, yl)), gets.at[7])
    arrived(first(xs, row_of(x + 2, 1 - yl)), gets.at[14])
    arrived(second(xs, row_of(x + 2, 1 - yl)), gets.at[15])
    arrived(first(zs, c_at(1 - yh, 2)), gets.at[16])
    arrived(second(zs, c_at(1 - yh, 2)), gets.at[17])
    share(c_at(1 - yh, 2), 7)

    def theirs(yh_, dz):
        return zs.at[col_of(yh_, z + dz, 1 - core)]

    order = [(yh, 0), (yh, 3), (yh, 1), (1 - yh, 0), (yh, 2), (1 - yh, 3), (1 - yh, 1), (1 - yh, 2)]
    for i, (yh_, dz) in enumerate(order):
        arrived(theirs(yh_, dz), sib_r.at[i])
    arrived(outgoing, store_sem)
    arrived(near, h_got)
    arrived(near.at[pl.ds(0, 127)], h_sent)
    for copy in open_sends:
        copy.wait_send()


def exchange(panels, local_h):
    any_space = pl.BlockSpec(memory_space=pl.ANY)
    dma = pltpu.SemaphoreType.DMA
    return pl.pallas_call(
        exchange_kernel,
        out_shape=(
            shape_of((16, 8, 3, BLOCK, 128)),
            shape_of((8, 16, BLOCK, 128)),
            shape_of((128, BLOCK, 128)),
            shape_of((8, 16, BLOCK, 128)),
        ),
        in_specs=[pl.BlockSpec(memory_space=pltpu.VMEM), any_space],
        out_specs=(any_space,) * 4,
        scratch_shapes=[
            pltpu.VMEM(local_h.shape, F32), dma((8,)), dma, dma((3,)),
            dma((2, 8)), dma((8,)), dma((16,)), dma((16,)), dma((18,)), dma((18,)), dma((8,)), dma((8,)),
            dma, dma,
        ],
        compiler_params=pltpu.CompilerParams(
            has_side_effects=True, vmem_limit_bytes=60 * 2**20
        ),
        cost_estimate=pl.CostEstimate(flops=0, bytes_accessed=64 * 2**20, transcendentals=0),
        name="exchange",
    )(panels, local_h)


def whole(shape):
    return pl.BlockSpec(shape, lambda *i: (0,) * len(shape), pipeline_mode=pl.Buffered(1))


SMEM = pl.BlockSpec(memory_space=pltpu.SMEM)
LIMIT = pltpu.CompilerParams(vmem_limit_bytes=60 * 2**20)


def shape_of(shape, dtype=F32):
    return jax.ShapeDtypeStruct(shape, dtype)


def per_device(h_old, s_old, row_owner, col_owner):
    rows_n = lax.axis_size("row")
    cols_n = lax.axis_size("col")
    row_id = lax.axis_index("row")
    col_id = lax.axis_index("col")
    place = jnp.stack([row_id, col_id]).astype(jnp.int32)
    local_h = h_old[0, 0]
    local_s = s_old[0, 0]
    band = ORDER // rows_n
    strip = ORDER // cols_n
    panels = jnp.concatenate([local_s, local_h[:, :BLOCK]], axis=1)
    band_tiles, strip_tiles, near, outgoing = exchange(panels.reshape(16, BLOCK, 128), local_h)
    far = lax.all_to_all(
        outgoing.reshape(rows_n * cols_n, BLOCK, 128), ("row", "col"), 0, 0, tiled=True
    )
    h_parts = [part.reshape(rows_n, cols_n, BLOCK, 128) for part in (near, far)]

    inverse, corner_h = pl.pallas_call(
        corner_kernel,
        out_shape=(shape_of((PANEL, PANEL)), shape_of((PANEL, PANEL))),
        grid=(1,),
        in_specs=[SMEM, SMEM, pl.BlockSpec((16, 8, 1, BLOCK, 128), lambda i: (0, 0, 2, 0, 0))],
        out_specs=(whole((PANEL, PANEL)),) * 2,
        scratch_shapes=[
            pltpu.VMEM((PANEL, PANEL), F32),
            pltpu.VMEM((PANEL // STEP, STEP, 2 * PANEL), F32),
            pltpu.VMEM((STEP, STEP), F32),
            pltpu.VMEM((STEP, STEP), F32),
        ],
        compiler_params=LIMIT,
        cost_estimate=pl.CostEstimate(flops=3 * 10**10, bytes_accessed=6 * 2**20, transcendentals=0),
        name="corner",
    )(row_owner, col_owner, band_tiles)

    buffers = [pltpu.VMEM((PANEL, PANEL), F32), pltpu.VMEM((PANEL, PANEL), F32)]
    right_high, right_low = pl.pallas_call(
        strip_kernel,
        grid=(strip // PANEL,),
        out_shape=(shape_of((strip, 2 * PANEL), BF16),) * 2,
        in_specs=[SMEM, SMEM, SMEM, whole(strip_tiles.shape), whole((PANEL, PANEL)), whole((PANEL, PANEL))],
        out_specs=(pl.BlockSpec((PANEL, 2 * PANEL), lambda i: (i, 0)),) * 2,
        scratch_shapes=buffers,
        compiler_params=LIMIT,
        cost_estimate=pl.CostEstimate(flops=10**10, bytes_accessed=10 * 2**20, transcendentals=0),
        name="strip",
    )(place, row_owner, col_owner, strip_tiles, inverse, corner_h)

    factor, left_high, left_low = pl.pallas_call(
        band_kernel,
        grid=(band // PANEL,),
        out_shape=(shape_of((band, PANEL)),) + (shape_of((band, 2 * PANEL), BF16),) * 2,
        in_specs=[SMEM, SMEM, SMEM, pl.BlockSpec((16, 8, 1, BLOCK, 128), lambda i: (0, 0, i // 2, 0, 0)), whole((PANEL, PANEL))],
        out_specs=(pl.BlockSpec((PANEL, PANEL), lambda i: (i, 0)),)
        + (pl.BlockSpec((PANEL, 2 * PANEL), lambda i: (i, 0)),) * 2,
        scratch_shapes=buffers,
        compiler_params=LIMIT,
        cost_estimate=pl.CostEstimate(flops=13 * 10**9, bytes_accessed=20 * 2**20, transcendentals=0),
        name="band",
    )(place, row_owner, col_owner, band_tiles, inverse)

    tall = 256
    count = band // tall // 2
    h_block = None
    for part in range(2):
        row_tile = lambda i, part=part: (i + part * count, 0)
        before = [] if h_block is None else [h_block]
        h_block = pl.pallas_call(
            functools.partial(final_kernel, part),
            grid=(count,),
            out_shape=shape_of((band, strip)),
            in_specs=[SMEM, SMEM, SMEM, whole(h_parts[part].shape)]
            + [pl.BlockSpec((tall, 2 * PANEL), row_tile)] * 2
            + [whole((strip, 2 * PANEL))] * 2
            + [pl.BlockSpec(memory_space=pl.ANY)] * len(before),
            out_specs=pl.BlockSpec((tall, strip), row_tile),
            input_output_aliases={8: 0} if before else {},
            compiler_params=LIMIT,
            cost_estimate=pl.CostEstimate(
                flops=65 * 10**8, bytes_accessed=14 * 2**20, transcendentals=0
            ),
            name=f"final_{part}",
        )(place, row_owner, col_owner, h_parts[part], left_high, left_low, right_high, right_low, *before)
    return h_block, factor


def solution(mesh):
    in_specs = (P("row", "col", None, None), P("row", "col", None, None), P(), P())
    out_specs = (P("row", "col"), P("row", None))
    return jax.shard_map(
        per_device, mesh=mesh, in_specs=in_specs, out_specs=out_specs, check_vma=False
    )
```

```python
import jax
import jax.numpy as jnp
from jax import lax
from jax.experimental import pallas as pl
from jax.experimental.pallas import tpu as pltpu
from jax.sharding import PartitionSpec as P

ORDER = 16384
PANEL = 512
BLOCK = 64
STEP = 128
FINE = 16
HIGHEST = lax.Precision.HIGHEST
BF16 = jnp.bfloat16
F32 = jnp.float32


def dot(a, b, ca, cb, precision=None):
    return lax.dot_general(
        a, b, (((ca,), (cb,)), ((), ())), precision=precision, preferred_element_type=F32
    )


def halves(x):
    high = x.astype(BF16)
    return high, (x - high.astype(F32)).astype(BF16)


def lower_half(shape):
    return lax.broadcasted_iota(jnp.int32, shape, 1) < BLOCK


def fetch_panel(read, rows, first, row_owner, col_owner, s_out, h_out):
    low = lower_half((BLOCK, 2 * BLOCK))
    for i in range(rows):
        p = row_owner[first + i]
        for k in range(0, PANEL // BLOCK, 2):
            one = read(i, p, col_owner[k])
            two = read(i, p, col_owner[k + 1])
            at = (pl.ds(i * BLOCK, BLOCK), pl.ds(k * BLOCK, 2 * BLOCK))
            s_out[at] = jnp.where(low, one, pltpu.roll(two, BLOCK, 1))
            h_out[at] = jnp.where(low, pltpu.roll(one, BLOCK, 1), two)


def spread(x, rows):
    return jnp.broadcast_to(x, (rows, x.shape[1]))


def factor_inverse(a_ref, b_ref):
    sub = lax.broadcasted_iota(jnp.int32, (8, STEP), 0)
    for j in range(0, STEP, 8):
        far = STEP - j - 8
        a_near, b_near = a_ref[j : j + 8, :], b_ref[j : j + 8, :]
        near = [jnp.broadcast_to(a_near[:, j + t : j + t + 1], (8, STEP)) for t in range(8)]
        if far:
            a_far, b_far = a_ref[j + 8 :, :], b_ref[j + 8 :, :]
            cols = [jnp.broadcast_to(a_far[:, j + t : j + t + 1], (far, STEP)) for t in range(8)]
        scales, links = [], []
        for t in range(8):
            r = lax.rsqrt(near[t][t : t + 1, :])
            l = near[t] * spread(r, 8)
            below = jnp.where(sub > t, l, 0.0)
            a_row, b_row = a_near[t : t + 1, :] * r, b_near[t : t + 1, :] * r
            a_near = jnp.where(sub == t, spread(a_row, 8), a_near - below * spread(a_row, 8))
            b_near = jnp.where(sub == t, spread(b_row, 8), b_near - below * spread(b_row, 8))
            link = {}
            for u in range(t + 1, 8):
                link[u] = l[u : u + 1, :]
                near[u] = near[u] - l * spread(link[u], 8)
            scales.append(r)
            links.append(link)
        b_ref[j : j + 8, :] = b_near
        if far:
            for t in range(8):
                l = cols[t] * spread(scales[t], far)
                for u in range(t + 1, 8):
                    cols[u] = cols[u] - l * spread(links[t][u], far)
                a_far = a_far - l * spread(a_near[t : t + 1, :], far)
                b_far = b_far - l * spread(b_near[t : t + 1, :], far)
            a_ref[j + 8 :, :] = a_far
            b_ref[j + 8 :, :] = b_far


def corner_kernel(row_owner, col_owner, tiles, inverse, corner_h, s_top, work, a_blk, b_blk):
    fetch_panel(
        lambda i, p, q: tiles[2 * q + p % 2, p // 2, 0],
        PANEL // BLOCK, 0, row_owner, col_owner, s_top, corner_h,
    )
    eye = lax.broadcasted_iota(jnp.int32, (STEP, STEP), 0) == lax.broadcasted_iota(
        jnp.int32, (STEP, STEP), 1
    )
    eye = jnp.where(eye, 1.0, 0.0)
    count = PANEL // STEP
    for k in range(count):
        work[k, :, :PANEL] = s_top[k * STEP : (k + 1) * STEP, :]
        work[k, :, PANEL:] = jnp.zeros((STEP, PANEL), F32)
        work[k, :, PANEL + k * STEP : PANEL + (k + 1) * STEP] = eye
    lane = lax.broadcasted_iota(jnp.int32, (STEP, PANEL), 1)

    def step(k, carry):
        a_blk[...] = work[k, :, pl.ds(pl.multiple_of(k * STEP, STEP), STEP)]
        b_blk[...] = eye
        factor_inverse(a_blk, b_blk)
        rows = dot(b_blk[...], work[k], 1, 0, HIGHEST)
        work[k] = rows
        ahead = jnp.where(lane >= (k + 1) * STEP, rows[:, :PANEL], 0.0).T
        for i in range(1, count):
            work[i] = work[i] - dot(ahead[i * STEP : (i + 1) * STEP], rows, 1, 0, HIGHEST)
        return carry

    lax.fori_loop(0, count, step, 0)
    for k in range(count):
        inverse[k * STEP : (k + 1) * STEP, :] = work[k, :, PANEL:]


def coupling_of(s_rows, inverse, special):
    factor = dot(s_rows, inverse, 1, 1, HIGHEST)
    coupling = dot(factor, inverse, 1, 0, HIGHEST)
    shape = (PANEL, PANEL)
    eye = lax.broadcasted_iota(jnp.int32, shape, 0) == lax.broadcasted_iota(jnp.int32, shape, 1)
    return factor, jnp.where(special, jnp.where(eye, 1.0, 0.0) - inverse, coupling)


def strip_kernel(place, row_owner, col_owner, tiles, inv, corner_h, high, low, s_buf, h_buf):
    step = pl.program_id(0)
    here = place[1]
    fetch_panel(
        lambda i, p, q: tiles[p // 2, 2 * q + p % 2],
        PANEL // BLOCK, here * 16 + step * 8, row_owner, col_owner, s_buf, h_buf,
    )
    special = jnp.logical_and(here == 0, step == 0)
    _, coupling = coupling_of(s_buf[...], inv[...], special)
    rest = h_buf[...] - dot(coupling, corner_h[...], 1, 0, HIGHEST)
    high[:, :PANEL], low[:, :PANEL] = halves(rest)
    high[:, PANEL:], low[:, PANEL:] = halves(coupling)


def band_kernel(place, row_owner, col_owner, tiles, inv, factor, high, low, s_buf, h_buf):
    step = pl.program_id(0)
    here = place[0]
    fetch_panel(
        lambda i, p, q: tiles[2 * q + p % 2, p // 2, 0],
        PANEL // BLOCK, here * 32 + step * 8, row_owner, col_owner, s_buf, h_buf,
    )
    special = jnp.logical_and(here == 0, step == 0)
    factor[...], coupling = coupling_of(s_buf[...], inv[...], special)
    high[:, :PANEL], low[:, :PANEL] = halves(coupling)
    high[:, PANEL:], low[:, PANEL:] = halves(h_buf[...])


def update_kernel(lh, ll, rh, rl, out):
    update = dot(lh[...], rh[...], 1, 1)
    update = update + dot(lh[...], rl[...], 1, 1)
    out[...] = update + dot(ll[...], rh[...], 1, 1)


def final_kernel(place, row_owner, col_owner, tiles, update, out):
    slot = pl.program_id(0)
    low = lower_half((FINE, 2 * BLOCK))
    owners = [col_owner[place[1] * 16 + j] * 2 for j in range(16)]
    for i in range(16):
        p = row_owner[place[0] * 32 + slot * 16 + i]
        for j in range(0, 16, 2):
            one = tiles[p // 2, owners[j] + p % 2]
            two = tiles[p // 2, owners[j + 1] + p % 2]
            if j < 8:
                both = jnp.where(low, one, pltpu.roll(two, BLOCK, 1))
            else:
                both = jnp.where(low, pltpu.roll(one, BLOCK, 1), two)
            at = (i, 0, slice(None), pl.ds(j * BLOCK, 2 * BLOCK))
            out[at] = both - update[at]


def axis_split(r, c):
    return r // 2, r % 2, c // 8, (c // 2) % 4, c % 2


def exchange_kernel(panels, h_ref, zs, xs, outgoing, h_buf, load_sem, store_sem, own_sem,
                    p1s, p1z, p1t, p1x, sends, gets, sib_s, sib_r):
    r, c = lax.axis_index("row"), lax.axis_index("col")
    x, yl, yh, z, core = axis_split(r, c)
    half_r, half_c = zs.shape[1] // 2, xs.shape[1] // 2

    def col_of(yh_, z_, core_):
        return yh_ * 8 + (z_ % 4) * 2 + core_

    def row_of(x_, yl_):
        return (x_ % 4) * 2 + yl_

    barrier = pltpu.get_barrier_semaphore()
    for d in range(1, 8):
        pl.semaphore_signal(barrier, inc=1, device_id=((r + d) % 8, c), device_id_type=pl.DeviceIdType.MESH)
    for d in range(1, 16):
        pl.semaphore_signal(barrier, inc=1, device_id=(r, (c + d) % 16), device_id_type=pl.DeviceIdType.MESH)
    loads = []
    for i in range(8):
        rows = pl.ds(i * 128, 128)
        loads.append(pltpu.make_async_copy(h_ref.at[rows], h_buf.at[rows], load_sem.at[i]))
        loads[-1].start()
    pl.semaphore_wait(barrier, 22)

    def send(src, dst, ss, rs, to):
        copy = pltpu.make_async_remote_copy(
            src_ref=src, dst_ref=dst, send_sem=ss, recv_sem=rs, device_id=to,
            device_id_type=pl.DeviceIdType.MESH,
        )
        copy.start()
        return copy

    def arrived(ref, sem):
        pltpu.make_async_copy(ref, ref, sem).wait()

    open_sends = []
    for d in range(1, 8):
        to = (r + d) % 8
        open_sends.append(send(panels.at[0], zs.at[c, r, 2], p1s.at[0, d], p1z.at[d], (to, c)))
        open_sends.append(
            send(panels.at[pl.ds(2 * to, 2)], zs.at[c, r, pl.ds(0, 2)], p1s.at[1, d], p1z.at[d], (to, c))
        )
    for d in range(1, 16):
        to = (c + d) % 16
        open_sends.append(send(panels.at[to], xs.at[r, c], p1t.at[d], p1x.at[d], (r, to)))
    own = [
        pltpu.make_async_copy(panels.at[0], zs.at[c, r, 2], own_sem.at[0]),
        pltpu.make_async_copy(panels.at[pl.ds(2 * r, 2)], zs.at[c, r, pl.ds(0, 2)], own_sem.at[1]),
        pltpu.make_async_copy(panels.at[c], xs.at[r, c], own_sem.at[2]),
    ]
    for copy in own:
        copy.start()

    zp, zm = (r, col_of(yh, z + 1, core)), (r, col_of(yh, z + 3, core))
    yp, sib = (r, col_of(1 - yh, z, core)), (r, col_of(yh, z, 1 - core))
    xp, xm, lp = (row_of(x + 1, yl), c), (row_of(x + 3, yl), c), (row_of(x, 1 - yl), c)

    def chunk_z(k):
        return zs.at[k]

    def chunk_x(k):
        return xs.at[k]

    def first(ref, k):
        return ref.at[k, pl.ds(0, ref.shape[1] // 2)]

    def second(ref, k):
        return ref.at[k, pl.ds(ref.shape[1] // 2, ref.shape[1] // 2)]

    def out(ref, i, to):
        open_sends.append(send(ref, ref, sends.at[i], gets.at[i], to))

    def share(k, i):
        open_sends.append(send(zs.at[k], zs.at[k], sib_s.at[i], sib_r.at[i], sib))

    own[0].wait()
    own[1].wait()
    for d in range(1, 8):
        arrived(zs.at[c, (r + 8 - d) % 8], p1z.at[d])
    out(chunk_z(c), 0, yp)
    out(chunk_z(c), 1, zp)
    out(chunk_z(c), 2, zm)
    own[2].wait()
    for d in range(1, 16):
        arrived(xs.at[r, (c + 16 - d) % 16], p1x.at[d])
    out(chunk_x(r), 3, lp)
    out(chunk_x(r), 4, xp)
    out(chunk_x(r), 5, xm)
    share(c, 0)

    for i in range(8):
        loads[i].wait()

    def tile(n, carry):
        i, j = n // 16, n % 16
        columns = pl.ds(pl.multiple_of(j * 128, 128), 128)
        rows = pl.ds(pl.multiple_of(i * 128, 128), 128)
        pltpu.make_async_copy(h_buf.at[rows, columns], outgoing.at[i, j], store_sem).start()
        return carry

    lax.fori_loop(0, 128, tile, 0)

    def c_at(yh_, dz):
        return col_of(yh_, z + dz, core)

    arrived(chunk_x(row_of(x + 3, yl)), gets.at[4])
    out(first(xs, row_of(x + 3, yl)), 6, xp)
    arrived(chunk_x(row_of(x + 1, yl)), gets.at[5])
    out(second(xs, row_of(x + 1, yl)), 7, xm)
    arrived(chunk_x(row_of(x, 1 - yl)), gets.at[3])
    out(chunk_x(row_of(x, 1 - yl)), 8, xp)
    out(chunk_x(row_of(x, 1 - yl)), 9, xm)

    arrived(chunk_z(c_at(yh, 3)), gets.at[1])
    out(first(zs, c_at(yh, 3)), 10, zp)
    arrived(chunk_z(c_at(yh, 1)), gets.at[2])
    out(second(zs, c_at(yh, 1)), 11, zm)
    arrived(chunk_z(c_at(1 - yh, 0)), gets.at[0])
    out(chunk_z(c_at(1 - yh, 0)), 12, zp)
    out(chunk_z(c_at(1 - yh, 0)), 13, zm)
    share(c_at(yh, 3), 1)
    share(c_at(yh, 1), 2)
    share(c_at(1 - yh, 0), 3)

    arrived(chunk_x(row_of(x + 3, 1 - yl)), gets.at[8])
    out(first(xs, row_of(x + 3, 1 - yl)), 14, xp)
    arrived(chunk_x(row_of(x + 1, 1 - yl)), gets.at[9])
    out(second(xs, row_of(x + 1, 1 - yl)), 15, xm)

    arrived(first(zs, c_at(yh, 2)), gets.at[10])
    arrived(second(zs, c_at(yh, 2)), gets.at[11])
    share(c_at(yh, 2), 4)
    arrived(chunk_z(c_at(1 - yh, 3)), gets.at[12])
    out(first(zs, c_at(1 - yh, 3)), 16, zp)
    arrived(chunk_z(c_at(1 - yh, 1)), gets.at[13])
    out(second(zs, c_at(1 - yh, 1)), 17, zm)
    share(c_at(1 - yh, 3), 5)
    share(c_at(1 - yh, 1), 6)

    arrived(first(xs, row_of(x + 2, yl)), gets.at[6])
    arrived(second(xs, row_of(x + 2, yl)), gets.at[7])
    arrived(first(xs, row_of(x + 2, 1 - yl)), gets.at[14])
    arrived(second(xs, row_of(x + 2, 1 - yl)), gets.at[15])
    arrived(first(zs, c_at(1 - yh, 2)), gets.at[16])
    arrived(second(zs, c_at(1 - yh, 2)), gets.at[17])
    share(c_at(1 - yh, 2), 7)

    def theirs(yh_, dz):
        return zs.at[col_of(yh_, z + dz, 1 - core)]

    order = [(yh, 0), (yh, 3), (yh, 1), (1 - yh, 0), (yh, 2), (1 - yh, 3), (1 - yh, 1), (1 - yh, 2)]
    for i, (yh_, dz) in enumerate(order):
        arrived(theirs(yh_, dz), sib_r.at[i])
    arrived(outgoing, store_sem)
    for copy in open_sends:
        copy.wait_send()


def exchange(panels, local_h):
    any_space = pl.BlockSpec(memory_space=pl.ANY)
    dma = pltpu.SemaphoreType.DMA
    return pl.pallas_call(
        exchange_kernel,
        out_shape=(
            shape_of((16, 8, 3, BLOCK, 128)),
            shape_of((8, 16, BLOCK, 128)),
            shape_of((8, 16, 128, 128)),
        ),
        in_specs=[pl.BlockSpec(memory_space=pltpu.VMEM), any_space],
        out_specs=(any_space,) * 3,
        scratch_shapes=[
            pltpu.VMEM(local_h.shape, F32), dma((8,)), dma, dma((3,)),
            dma((2, 8)), dma((8,)), dma((16,)), dma((16,)), dma((18,)), dma((18,)), dma((8,)), dma((8,)),
        ],
        compiler_params=pltpu.CompilerParams(
            collective_id=0, has_side_effects=True, vmem_limit_bytes=60 * 2**20
        ),
        cost_estimate=pl.CostEstimate(flops=0, bytes_accessed=64 * 2**20, transcendentals=0),
        name="exchange",
    )(panels, local_h)


def whole(shape):
    return pl.BlockSpec(shape, lambda *i: (0,) * len(shape), pipeline_mode=pl.Buffered(1))


SMEM = pl.BlockSpec(memory_space=pltpu.SMEM)
LIMIT = pltpu.CompilerParams(vmem_limit_bytes=60 * 2**20)


def shape_of(shape, dtype=F32):
    return jax.ShapeDtypeStruct(shape, dtype)


def per_device(h_old, s_old, row_owner, col_owner):
    rows_n = lax.axis_size("row")
    cols_n = lax.axis_size("col")
    row_id = lax.axis_index("row")
    col_id = lax.axis_index("col")
    place = jnp.stack([row_id, col_id]).astype(jnp.int32)
    local_h = h_old[0, 0]
    local_s = s_old[0, 0]
    band = ORDER // rows_n
    strip = ORDER // cols_n
    panels = jnp.concatenate([local_s, local_h[:, :BLOCK]], axis=1)
    band_tiles, strip_tiles, outgoing = exchange(panels.reshape(16, BLOCK, 128), local_h)
    h_tiles = lax.all_to_all(
        outgoing.reshape(rows_n * cols_n, 128, 128), ("row", "col"), 0, 0, tiled=True
    ).reshape(rows_n, cols_n, 128, 128)

    inverse, corner_h = pl.pallas_call(
        corner_kernel,
        out_shape=(shape_of((PANEL, PANEL)), shape_of((PANEL, PANEL))),
        grid=(1,),
        in_specs=[SMEM, SMEM, pl.BlockSpec((16, 8, 1, BLOCK, 128), lambda i: (0, 0, 2, 0, 0))],
        out_specs=(whole((PANEL, PANEL)),) * 2,
        scratch_shapes=[
            pltpu.VMEM((PANEL, PANEL), F32),
            pltpu.VMEM((PANEL // STEP, STEP, 2 * PANEL), F32),
            pltpu.VMEM((STEP, STEP), F32),
            pltpu.VMEM((STEP, STEP), F32),
        ],
        compiler_params=LIMIT,
        cost_estimate=pl.CostEstimate(flops=3 * 10**10, bytes_accessed=6 * 2**20, transcendentals=0),
        name="corner",
    )(row_owner, col_owner, band_tiles)

    buffers = [pltpu.VMEM((PANEL, PANEL), F32), pltpu.VMEM((PANEL, PANEL), F32)]
    right_high, right_low = pl.pallas_call(
        strip_kernel,
        grid=(strip // PANEL,),
        out_shape=(shape_of((strip, 2 * PANEL), BF16),) * 2,
        in_specs=[SMEM, SMEM, SMEM, whole(strip_tiles.shape), whole((PANEL, PANEL)), whole((PANEL, PANEL))],
        out_specs=(pl.BlockSpec((PANEL, 2 * PANEL), lambda i: (i, 0)),) * 2,
        scratch_shapes=buffers,
        compiler_params=LIMIT,
        cost_estimate=pl.CostEstimate(flops=10**10, bytes_accessed=10 * 2**20, transcendentals=0),
        name="strip",
    )(place, row_owner, col_owner, strip_tiles, inverse, corner_h)

    factor, left_high, left_low = pl.pallas_call(
        band_kernel,
        grid=(band // PANEL,),
        out_shape=(shape_of((band, PANEL)),) + (shape_of((band, 2 * PANEL), BF16),) * 2,
        in_specs=[SMEM, SMEM, SMEM, pl.BlockSpec((16, 8, 1, BLOCK, 128), lambda i: (0, 0, i // 2, 0, 0)), whole((PANEL, PANEL))],
        out_specs=(pl.BlockSpec((PANEL, PANEL), lambda i: (i, 0)),)
        + (pl.BlockSpec((PANEL, 2 * PANEL), lambda i: (i, 0)),) * 2,
        scratch_shapes=buffers,
        compiler_params=LIMIT,
        cost_estimate=pl.CostEstimate(flops=13 * 10**9, bytes_accessed=20 * 2**20, transcendentals=0),
        name="band",
    )(place, row_owner, col_owner, band_tiles, inverse)

    tall = 256
    update = pl.pallas_call(
        update_kernel,
        grid=(band // tall,),
        out_shape=shape_of((band, strip)),
        in_specs=[pl.BlockSpec((tall, 2 * PANEL), lambda i: (i, 0))] * 2
        + [whole((strip, 2 * PANEL))] * 2,
        out_specs=pl.BlockSpec((tall, strip), lambda i: (i, 0)),
        compiler_params=pltpu.CompilerParams(vmem_limit_bytes=60 * 2**20),
        cost_estimate=pl.CostEstimate(flops=13 * 10**9, bytes_accessed=20 * 2**20, transcendentals=0),
        name="update",
    )(left_high, left_low, right_high, right_low)

    fine = pl.BlockSpec((16, 1, FINE, strip), lambda s, u: (s, u, 0, 0))
    h_block = pl.pallas_call(
        final_kernel,
        grid=(2, BLOCK // FINE),
        out_shape=shape_of((band // BLOCK, BLOCK // FINE, FINE, strip)),
        in_specs=[
            SMEM, SMEM, SMEM,
            pl.BlockSpec((rows_n, cols_n, FINE, 128), lambda s, u: (0, 0, s * (BLOCK // FINE) + u, 0)),
            fine,
        ],
        out_specs=fine,
        compiler_params=pltpu.CompilerParams(vmem_limit_bytes=60 * 2**20),
        cost_estimate=pl.CostEstimate(flops=2**22, bytes_accessed=24 * 2**20, transcendentals=0),
        name="final",
    )(place, row_owner, col_owner, h_tiles, update.reshape(band // BLOCK, BLOCK // FINE, FINE, strip))
    return h_block.reshape(band, strip), factor


def solution(mesh):
    in_specs = (P("row", "col", None, None), P("row", "col", None, None), P(), P())
    out_specs = (P("row", "col"), P("row", None))
    return jax.shard_map(
        per_device, mesh=mesh, in_specs=in_specs, out_specs=out_specs, check_vma=False
    )
```

```python
import jax
import jax.numpy as jnp
from jax import lax
from jax.experimental import pallas as pl
from jax.experimental.pallas import tpu as pltpu
from jax.sharding import PartitionSpec as P

ORDER = 16384
PANEL = 512
BLOCK = 64
STEP = 128
FINE = 16
TALL = 256
EARLY = 16
HIGHEST = lax.Precision.HIGHEST
BF16 = jnp.bfloat16
F32 = jnp.float32


def dot(a, b, ca, cb, precision=None):
    return lax.dot_general(
        a, b, (((ca,), (cb,)), ((), ())), precision=precision, preferred_element_type=F32
    )


def halves(x):
    high = x.astype(BF16)
    return high, (x - high.astype(F32)).astype(BF16)


def lower_half(shape):
    return lax.broadcasted_iota(jnp.int32, shape, 1) < BLOCK


def fetch_panel(read, rows, first, row_owner, col_owner, s_out, h_out):
    low = lower_half((BLOCK, 2 * BLOCK))
    for i in range(rows):
        p = row_owner[first + i]
        for k in range(0, PANEL // BLOCK, 2):
            one = read(i, p, col_owner[k])
            two = read(i, p, col_owner[k + 1])
            at = (pl.ds(i * BLOCK, BLOCK), pl.ds(k * BLOCK, 2 * BLOCK))
            s_out[at] = jnp.where(low, one, pltpu.roll(two, BLOCK, 1))
            h_out[at] = jnp.where(low, pltpu.roll(one, BLOCK, 1), two)


def spread(x, rows):
    return jnp.broadcast_to(x, (rows, x.shape[1]))


def factor_inverse(a_ref, b_ref):
    sub = lax.broadcasted_iota(jnp.int32, (8, STEP), 0)
    for j in range(0, STEP, 8):
        far = STEP - j - 8
        a_near, b_near = a_ref[j : j + 8, :], b_ref[j : j + 8, :]
        near = [jnp.broadcast_to(a_near[:, j + t : j + t + 1], (8, STEP)) for t in range(8)]
        if far:
            a_far, b_far = a_ref[j + 8 :, :], b_ref[j + 8 :, :]
            cols = [jnp.broadcast_to(a_far[:, j + t : j + t + 1], (far, STEP)) for t in range(8)]
        scales, links = [], []
        for t in range(8):
            r = lax.rsqrt(near[t][t : t + 1, :])
            l = near[t] * spread(r, 8)
            below = jnp.where(sub > t, l, 0.0)
            a_row, b_row = a_near[t : t + 1, :] * r, b_near[t : t + 1, :] * r
            a_near = jnp.where(sub == t, spread(a_row, 8), a_near - below * spread(a_row, 8))
            b_near = jnp.where(sub == t, spread(b_row, 8), b_near - below * spread(b_row, 8))
            link = {}
            for u in range(t + 1, 8):
                link[u] = l[u : u + 1, :]
                near[u] = near[u] - l * spread(link[u], 8)
            scales.append(r)
            links.append(link)
        b_ref[j : j + 8, :] = b_near
        if far:
            for t in range(8):
                l = cols[t] * spread(scales[t], far)
                for u in range(t + 1, 8):
                    cols[u] = cols[u] - l * spread(links[t][u], far)
                a_far = a_far - l * spread(a_near[t : t + 1, :], far)
                b_far = b_far - l * spread(b_near[t : t + 1, :], far)
            a_ref[j + 8 :, :] = a_far
            b_ref[j + 8 :, :] = b_far


def corner_inverse(s_top, work, a_blk, b_blk, inverse):
    eye = lax.broadcasted_iota(jnp.int32, (STEP, STEP), 0) == lax.broadcasted_iota(
        jnp.int32, (STEP, STEP), 1
    )
    eye = jnp.where(eye, 1.0, 0.0)
    count = PANEL // STEP
    for k in range(count):
        work[k, :, :PANEL] = s_top[k * STEP : (k + 1) * STEP, :]
        work[k, :, PANEL:] = jnp.zeros((STEP, PANEL), F32)
        work[k, :, PANEL + k * STEP : PANEL + (k + 1) * STEP] = eye
    lane = lax.broadcasted_iota(jnp.int32, (STEP, PANEL), 1)

    def step(k, carry):
        a_blk[...] = work[k, :, pl.ds(pl.multiple_of(k * STEP, STEP), STEP)]
        b_blk[...] = eye
        factor_inverse(a_blk, b_blk)
        rows = dot(b_blk[...], work[k], 1, 0, HIGHEST)
        work[k] = rows
        ahead = jnp.where(lane >= (k + 1) * STEP, rows[:, :PANEL], 0.0).T
        for i in range(1, count):
            work[i] = work[i] - dot(ahead[i * STEP : (i + 1) * STEP], rows, 1, 0, HIGHEST)
        return carry

    lax.fori_loop(0, count, step, 0)
    for k in range(count):
        inverse[k * STEP : (k + 1) * STEP, :] = work[k, :, PANEL:]


def coupling_of(s_rows, inv, special, step):
    inverse = inv[...]
    factor = dot(s_rows, inverse, 1, 1, HIGHEST)
    coupling = dot(factor, inverse, 1, 0, HIGHEST)
    at = pl.multiple_of(lax.rem(step, 2) * TALL, TALL)
    shape = (TALL, PANEL)
    eye = at + lax.broadcasted_iota(jnp.int32, shape, 0) == lax.broadcasted_iota(jnp.int32, shape, 1)
    top = jnp.where(eye, 1.0, 0.0) - inv[pl.ds(at, TALL), :]
    return factor, jnp.where(special, top, coupling)


def final_kernel(place, row_owner, col_owner, tiles, update, out):
    slot = pl.program_id(0)
    low = lower_half((FINE, 2 * BLOCK))
    owners = [col_owner[place[1] * 16 + j] * 2 for j in range(16)]
    for i in range(16):
        p = row_owner[place[0] * 32 + slot * 16 + i]
        for j in range(0, 16, 2):
            one = tiles[p // 2, owners[j] + p % 2]
            two = tiles[p // 2, owners[j + 1] + p % 2]
            if j < 8:
                both = jnp.where(low, one, pltpu.roll(two, BLOCK, 1))
            else:
                both = jnp.where(low, pltpu.roll(one, BLOCK, 1), two)
            at = (i, 0, slice(None), pl.ds(j * BLOCK, 2 * BLOCK))
            out[at] = both - update[at]


def axis_split(r, c):
    return r // 2, r % 2, c // 8, (c // 2) % 4, c % 2


def panel_kernel(panels, stored, h_ref, row_owner, col_owner, near, update, factor,
                 zs, cs, cp, xs, work, a_blk, b_blk, inv, corner_h, s_buf, h_buf,
                 rh, rl, lh, ll, f_buf, u_buf,
                 own_sem, p1a, p1a_got, p1x, p1x_got, p1c, p1c_got, sends, gets,
                 sib_a, sib_a_got, sib_c, sib_c_got, h_sent, h_got, out_sem):
    r, c = lax.axis_index("row"), lax.axis_index("col")
    x, yl, yh, z, core = axis_split(r, c)

    def col_of(yh_, z_, core_):
        return yh_ * 8 + (z_ % 4) * 2 + core_

    def row_of(x_, yl_):
        return (x_ % 4) * 2 + yl_

    open_sends = []

    def send(src, dst, ss, rs, to):
        copy = pltpu.make_async_remote_copy(
            src_ref=src, dst_ref=dst, send_sem=ss, recv_sem=rs, device_id=to,
            device_id_type=pl.DeviceIdType.MESH,
        )
        copy.start()
        open_sends.append(copy)

    def arrived(ref, sem):
        pltpu.make_async_copy(ref, ref, sem).wait()

    own = [
        pltpu.make_async_copy(stored.at[pl.ds(2 * r, 2)], zs.at[c, r], own_sem.at[0]),
        pltpu.make_async_copy(stored.at[c], xs.at[r, c], own_sem.at[1]),
        pltpu.make_async_copy(stored.at[0], cp.at[core, r], own_sem.at[2]),
    ]
    for copy in own:
        copy.start()
    for d in range(1, 8):
        to = (r + d) % 8
        send(panels.at[pl.ds(2 * to, 2)], zs.at[c, r], p1a.at[d], p1a_got.at[d], (to, c))
    for d in range(1, 16):
        to = (c + d) % 16
        send(panels.at[to], xs.at[r, c], p1x.at[d], p1x_got.at[d], (r, to))
    for d in range(1, 8):
        send(panels.at[0], cp.at[core, r], p1c.at[d], p1c_got.at[d], ((r + d) % 8, c))

    def h_tile(i, j):
        rows = pl.ds(pl.multiple_of(i * 128, 128), 128)
        return h_ref.at[rows, pl.ds(pl.multiple_of(j * 128, 128), 128)]

    def send_tile(n, carry):
        i, j = (r + n % 8) % 8, (c + n // 8) % 16
        pltpu.make_async_remote_copy(
            src_ref=h_tile(i, j), dst_ref=near.at[r * 16 + c], send_sem=h_sent, recv_sem=h_got,
            device_id=(i, j), device_id_type=pl.DeviceIdType.MESH,
        ).start()
        return carry

    lax.fori_loop(1, EARLY, send_tile, 0)

    zp, zm = (r, col_of(yh, z + 1, core)), (r, col_of(yh, z + 3, core))
    yp, sib = (r, col_of(1 - yh, z, core)), (r, col_of(yh, z, 1 - core))
    xp, xm, lp = (row_of(x + 1, yl), c), (row_of(x + 3, yl), c), (row_of(x, 1 - yl), c)

    def ring(ref, base, index, side, ahead, behind):
        half = ref.shape[1] // 2
        first = lambda k: ref.at[k, pl.ds(0, half)]
        second = lambda k: ref.at[k, pl.ds(half, half)]

        def out(piece, i, to):
            send(piece, piece, sends.at[base + i], gets.at[base + i], to)

        def start():
            mine = index(0, 0)
            out(ref.at[mine], 0, side)
            out(ref.at[mine], 1, ahead)
            out(ref.at[mine], 2, behind)

        def onward(plane):
            i = 1 + 4 * plane
            arrived(ref.at[index(plane, 3)], gets.at[base + i])
            out(first(index(plane, 3)), i + 2, ahead)
            arrived(ref.at[index(plane, 1)], gets.at[base + i + 1])
            out(second(index(plane, 1)), i + 3, behind)

        def beside():
            other = index(1, 0)
            arrived(ref.at[other], gets.at[base])
            out(ref.at[other], 5, ahead)
            out(ref.at[other], 6, behind)

        def last(plane):
            i = 3 + 4 * plane
            arrived(first(index(plane, 2)), gets.at[base + i])
            arrived(second(index(plane, 2)), gets.at[base + i + 1])

        return start, onward, beside, last

    def col_index(plane, d):
        return col_of(yh if plane == 0 else 1 - yh, z + d, core)

    def row_index(plane, d):
        return row_of(x + d, yl if plane == 0 else 1 - yl)

    start_a, onward_a, beside_a, last_a = ring(zs, 0, col_index, yp, zp, zm)
    start_x, onward_x, beside_x, last_x = ring(xs, 9, row_index, lp, xp, xm)
    start_c, onward_c, beside_c, last_c = ring(cs, 18, col_index, yp, zp, zm)
    shares = [(0, 0), (0, 3), (0, 1), (1, 0), (1, 3), (1, 1), (0, 2), (1, 2)]

    def share(ref, ss, rs, i):
        piece = ref.at[col_index(*shares[i])]
        send(piece, piece, ss.at[i], rs.at[i], sib)

    def shared(ref, rs, i):
        plane, d = shares[i]
        arrived(ref.at[col_of(yh if plane == 0 else 1 - yh, z + d, 1 - core)], rs.at[i])

    own[0].wait()
    for d in range(1, 8):
        arrived(zs.at[c, (r + 8 - d) % 8], p1a_got.at[d])
    start_a()
    own[1].wait()
    for d in range(1, 16):
        arrived(xs.at[r, (c + 16 - d) % 16], p1x_got.at[d])
    start_x()
    own[2].wait()
    for d in range(1, 8):
        arrived(cp.at[core, (r + 8 - d) % 8], p1c_got.at[d])
    send(cp.at[core], cp.at[core], p1c.at[0], p1c_got.at[0], sib)
    arrived(cp.at[1 - core], p1c_got.at[0])
    for i in range(4):
        p = row_owner[4 * core + i]
        cs[c, i] = cp[p % 2, p // 2]
    share(zs, sib_a, sib_a_got, 0)
    start_c()
    share(cs, sib_c, sib_c_got, 0)
    onward_x(0)
    onward_a(0)
    beside_x()
    beside_a()
    onward_c(0)
    beside_c()
    for i in range(1, 4):
        share(zs, sib_a, sib_a_got, i)
        share(cs, sib_c, sib_c_got, i)
    onward_x(1)
    onward_a(1)
    onward_c(1)
    lax.fori_loop(EARLY, 128, send_tile, 0)
    kept = pltpu.make_async_copy(h_tile(r, c), near.at[r * 16 + c], h_got)
    kept.start()
    for i in range(4, 6):
        share(cs, sib_c, sib_c_got, i)
        share(zs, sib_a, sib_a_got, i)
    last_a(0)
    share(zs, sib_a, sib_a_got, 6)
    last_c(0)
    share(cs, sib_c, sib_c_got, 6)
    last_c(1)
    share(cs, sib_c, sib_c_got, 7)
    for i in range(8):
        shared(cs, sib_c_got, i)

    fetch_panel(
        lambda i, p, q: cs[2 * q + i // 4, i % 4],
        PANEL // BLOCK, 0, row_owner, col_owner, s_buf, corner_h,
    )
    corner_inverse(s_buf, work, a_blk, b_blk, inv)
    last_a(1)
    share(zs, sib_a, sib_a_got, 7)
    for plane in range(2):
        last_x(plane)

    def strip_step(t, carry):
        fetch_panel(
            lambda i, p, q: xs[p // 2, 2 * q + p % 2],
            TALL // BLOCK, c * 16 + t * 4, row_owner, col_owner, s_buf, h_buf,
        )
        special = jnp.logical_and(c == 0, t < 2)
        _, coupling = coupling_of(s_buf[:TALL, :], inv, special, t)
        rest = h_buf[...] - dot(coupling, corner_h[...], 1, 0, HIGHEST)
        at = pl.ds(pl.multiple_of(t * TALL, TALL), TALL)
        rh[at, :PANEL], rl[at, :PANEL] = halves(rest)
        rh[at, PANEL:], rl[at, PANEL:] = halves(coupling)
        return carry

    lax.fori_loop(0, rh.shape[0] // TALL, strip_step, 0)
    for i in range(8):
        shared(zs, sib_a_got, i)

    def rows_of(t):
        return pl.ds(pl.multiple_of(t * TALL, TALL), TALL)

    def band_step(t, carry):
        slot = t // 4
        fetch_panel(
            lambda i, p, q: zs[2 * q + p % 2, p // 2, slot],
            TALL // BLOCK, r * 32 + t * 4, row_owner, col_owner, s_buf, h_buf,
        )
        special = jnp.logical_and(r == 0, t < 2)
        panel, coupling = coupling_of(s_buf[:TALL, :], inv, special, t)
        f_buf[rows_of(t), :] = panel
        lh[:, :PANEL], ll[:, :PANEL] = halves(coupling)
        lh[:, PANEL:], ll[:, PANEL:] = halves(h_buf[...])
        total = dot(lh[...], rh[...], 1, 1)
        total = total + dot(lh[...], rl[...], 1, 1)
        u_buf[rows_of(t), :] = total + dot(ll[...], rh[...], 1, 1)
        pltpu.make_async_copy(u_buf.at[rows_of(t)], update.at[rows_of(t)], out_sem.at[0, t]).start()
        pltpu.make_async_copy(f_buf.at[rows_of(t)], factor.at[rows_of(t)], out_sem.at[1, t]).start()
        return carry

    steps = u_buf.shape[0] // TALL
    lax.fori_loop(0, steps, band_step, 0)
    for t in range(steps):
        pltpu.make_async_copy(u_buf.at[rows_of(t)], update.at[rows_of(t)], out_sem.at[0, t]).wait()
        pltpu.make_async_copy(f_buf.at[rows_of(t)], factor.at[rows_of(t)], out_sem.at[1, t]).wait()
    arrived(near, h_got)
    arrived(near.at[pl.ds(0, 127)], h_sent)
    for copy in open_sends:
        copy.wait_send()


SMEM = pl.BlockSpec(memory_space=pltpu.SMEM)


def shape_of(shape, dtype=F32):
    return jax.ShapeDtypeStruct(shape, dtype)


def per_device(h_old, s_old, row_owner, col_owner):
    rows_n = lax.axis_size("row")
    cols_n = lax.axis_size("col")
    row_id = lax.axis_index("row")
    col_id = lax.axis_index("col")
    place = jnp.stack([row_id, col_id]).astype(jnp.int32)
    local_h = h_old[0, 0]
    local_s = s_old[0, 0]
    band = ORDER // rows_n
    strip = ORDER // cols_n
    panels = jnp.concatenate([local_s, local_h[:, :BLOCK]], axis=1).reshape(16, BLOCK, 128)
    any_space = pl.BlockSpec(memory_space=pl.ANY)
    dma = pltpu.SemaphoreType.DMA
    vmem = pltpu.VMEM
    near, update, factor = pl.pallas_call(
        panel_kernel,
        out_shape=(shape_of((128, 128, 128)), shape_of((band, strip)), shape_of((band, PANEL))),
        in_specs=[pl.BlockSpec(memory_space=pltpu.VMEM), any_space, any_space, SMEM, SMEM],
        out_specs=(any_space,) * 3,
        scratch_shapes=[
            vmem((16, 8, 2, BLOCK, 128), F32),
            vmem((16, 4, BLOCK, 128), F32),
            vmem((2, 8, BLOCK, 128), F32),
            vmem((8, 16, BLOCK, 128), F32),
            vmem((PANEL // STEP, STEP, 2 * PANEL), F32),
            vmem((STEP, STEP), F32),
            vmem((STEP, STEP), F32),
            vmem((PANEL, PANEL), F32),
            vmem((PANEL, PANEL), F32),
            vmem((PANEL, PANEL), F32),
            vmem((TALL, PANEL), F32),
            vmem((strip, 2 * PANEL), BF16),
            vmem((strip, 2 * PANEL), BF16),
            vmem((TALL, 2 * PANEL), BF16),
            vmem((TALL, 2 * PANEL), BF16),
            vmem((band, PANEL), F32),
            vmem((band, strip), F32),
            dma((3,)), dma((8,)), dma((8,)), dma((16,)), dma((16,)), dma((8,)), dma((8,)),
            dma((27,)), dma((27,)), dma((8,)), dma((8,)), dma((8,)), dma((8,)), dma, dma,
            dma((2, band // TALL)),
        ],
        compiler_params=pltpu.CompilerParams(has_side_effects=True, vmem_limit_bytes=60 * 2**20),
        cost_estimate=pl.CostEstimate(flops=4 * 10**10, bytes_accessed=64 * 2**20, transcendentals=0),
        name="panel",
    )(panels, panels, local_h, row_owner, col_owner)
    h_tiles = near.reshape(rows_n, cols_n, 128, 128)

    fine = pl.BlockSpec((16, 1, FINE, strip), lambda s, u: (s, u, 0, 0))
    h_block = pl.pallas_call(
        final_kernel,
        grid=(2, BLOCK // FINE),
        out_shape=shape_of((band // BLOCK, BLOCK // FINE, FINE, strip)),
        in_specs=[
            SMEM, SMEM, SMEM,
            pl.BlockSpec((rows_n, cols_n, FINE, 128), lambda s, u: (0, 0, s * (BLOCK // FINE) + u, 0)),
            fine,
        ],
        out_specs=fine,
        compiler_params=pltpu.CompilerParams(vmem_limit_bytes=60 * 2**20),
        cost_estimate=pl.CostEstimate(flops=2**22, bytes_accessed=24 * 2**20, transcendentals=0),
        name="final",
    )(place, row_owner, col_owner, h_tiles, update.reshape(band // BLOCK, BLOCK // FINE, FINE, strip))
    return h_block.reshape(band, strip), factor


def solution(mesh):
    in_specs = (P("row", "col", None, None), P("row", "col", None, None), P(), P())
    out_specs = (P("row", "col"), P("row", None))
    return jax.shard_map(
        per_device, mesh=mesh, in_specs=in_specs, out_specs=out_specs, check_vma=False
    )
```

```python
import jax
import jax.numpy as jnp
from jax import lax
from jax.experimental import pallas as pl
from jax.experimental.pallas import tpu as pltpu
from jax.sharding import PartitionSpec as P

ORDER = 16384
PANEL = 512
BLOCK = 64
STEP = 128
FINE = 16
TALL = 256
EARLY = 1
HIGHEST = lax.Precision.HIGHEST
BF16 = jnp.bfloat16
F32 = jnp.float32


def dot(a, b, ca, cb, precision=None):
    return lax.dot_general(
        a, b, (((ca,), (cb,)), ((), ())), precision=precision, preferred_element_type=F32
    )


def halves(x):
    high = x.astype(BF16)
    return high, (x - high.astype(F32)).astype(BF16)


def lower_half(shape):
    return lax.broadcasted_iota(jnp.int32, shape, 1) < BLOCK


def fetch_panel(read, rows, first, row_owner, col_owner, s_out, h_out):
    low = lower_half((BLOCK, 2 * BLOCK))
    for i in range(rows):
        p = row_owner[first + i]
        for k in range(0, PANEL // BLOCK, 2):
            one = read(i, p, col_owner[k])
            two = read(i, p, col_owner[k + 1])
            at = (pl.ds(i * BLOCK, BLOCK), pl.ds(k * BLOCK, 2 * BLOCK))
            s_out[at] = jnp.where(low, one, pltpu.roll(two, BLOCK, 1))
            h_out[at] = jnp.where(low, pltpu.roll(one, BLOCK, 1), two)


def spread(x, rows):
    return jnp.broadcast_to(x, (rows, x.shape[1]))


def factor_inverse(a_ref, b_ref):
    sub = lax.broadcasted_iota(jnp.int32, (8, STEP), 0)
    for j in range(0, STEP, 8):
        far = STEP - j - 8
        a_near, b_near = a_ref[j : j + 8, :], b_ref[j : j + 8, :]
        near = [jnp.broadcast_to(a_near[:, j + t : j + t + 1], (8, STEP)) for t in range(8)]
        if far:
            a_far, b_far = a_ref[j + 8 :, :], b_ref[j + 8 :, :]
            cols = [jnp.broadcast_to(a_far[:, j + t : j + t + 1], (far, STEP)) for t in range(8)]
        scales, links = [], []
        for t in range(8):
            r = lax.rsqrt(near[t][t : t + 1, :])
            l = near[t] * spread(r, 8)
            below = jnp.where(sub > t, l, 0.0)
            a_row, b_row = a_near[t : t + 1, :] * r, b_near[t : t + 1, :] * r
            a_near = jnp.where(sub == t, spread(a_row, 8), a_near - below * spread(a_row, 8))
            b_near = jnp.where(sub == t, spread(b_row, 8), b_near - below * spread(b_row, 8))
            link = {}
            for u in range(t + 1, 8):
                link[u] = l[u : u + 1, :]
                near[u] = near[u] - l * spread(link[u], 8)
            scales.append(r)
            links.append(link)
        b_ref[j : j + 8, :] = b_near
        if far:
            for t in range(8):
                l = cols[t] * spread(scales[t], far)
                for u in range(t + 1, 8):
                    cols[u] = cols[u] - l * spread(links[t][u], far)
                a_far = a_far - l * spread(a_near[t : t + 1, :], far)
                b_far = b_far - l * spread(b_near[t : t + 1, :], far)
            a_ref[j + 8 :, :] = a_far
            b_ref[j + 8 :, :] = b_far


def corner_inverse(s_top, work, a_blk, b_blk, inverse):
    eye = lax.broadcasted_iota(jnp.int32, (STEP, STEP), 0) == lax.broadcasted_iota(
        jnp.int32, (STEP, STEP), 1
    )
    eye = jnp.where(eye, 1.0, 0.0)
    count = PANEL // STEP
    for k in range(count):
        work[k, :, :PANEL] = s_top[k * STEP : (k + 1) * STEP, :]
        work[k, :, PANEL:] = jnp.zeros((STEP, PANEL), F32)
        work[k, :, PANEL + k * STEP : PANEL + (k + 1) * STEP] = eye
    lane = lax.broadcasted_iota(jnp.int32, (STEP, PANEL), 1)

    def step(k, carry):
        a_blk[...] = work[k, :, pl.ds(pl.multiple_of(k * STEP, STEP), STEP)]
        b_blk[...] = eye
        factor_inverse(a_blk, b_blk)
        rows = dot(b_blk[...], work[k], 1, 0, HIGHEST)
        work[k] = rows
        ahead = jnp.where(lane >= (k + 1) * STEP, rows[:, :PANEL], 0.0).T
        for i in range(1, count):
            work[i] = work[i] - dot(ahead[i * STEP : (i + 1) * STEP], rows, 1, 0, HIGHEST)
        return carry

    lax.fori_loop(0, count, step, 0)
    for k in range(count):
        inverse[k * STEP : (k + 1) * STEP, :] = work[k, :, PANEL:]


def coupling_of(s_rows, inv, special, step):
    inverse = inv[...]
    factor = dot(s_rows, inverse, 1, 1, HIGHEST)
    coupling = dot(factor, inverse, 1, 0, HIGHEST)
    at = pl.multiple_of(lax.rem(step, 2) * TALL, TALL)
    shape = (TALL, PANEL)
    eye = at + lax.broadcasted_iota(jnp.int32, shape, 0) == lax.broadcasted_iota(jnp.int32, shape, 1)
    top = jnp.where(eye, 1.0, 0.0) - inv[pl.ds(at, TALL), :]
    return factor, jnp.where(special, top, coupling)


def final_kernel(place, row_owner, col_owner, tiles, update, out):
    slot = pl.program_id(0)
    low = lower_half((FINE, 2 * BLOCK))
    owners = [col_owner[place[1] * 16 + j] * 2 for j in range(16)]
    for i in range(16):
        p = row_owner[place[0] * 32 + slot * 16 + i]
        for j in range(0, 16, 2):
            one = tiles[p // 2, owners[j] + p % 2]
            two = tiles[p // 2, owners[j + 1] + p % 2]
            if j < 8:
                both = jnp.where(low, one, pltpu.roll(two, BLOCK, 1))
            else:
                both = jnp.where(low, pltpu.roll(one, BLOCK, 1), two)
            at = (i, 0, slice(None), pl.ds(j * BLOCK, 2 * BLOCK))
            out[at] = both - update[at]


def axis_split(r, c):
    return r // 2, r % 2, c // 8, (c // 2) % 4, c % 2


def panel_kernel(panels, stored, h_ref, row_owner, col_owner, near, update, factor,
                 zs, cs, cp, xs, work, a_blk, b_blk, inv, corner_h, s_buf, h_buf,
                 rh, rl, lh, ll, f_buf, u_buf,
                 own_sem, p1a, p1a_got, p1x, p1x_got, p1c, p1c_got, sends, gets,
                 sib_a, sib_a_got, sib_c, sib_c_got, h_sent, h_got, out_sem):
    r, c = lax.axis_index("row"), lax.axis_index("col")
    x, yl, yh, z, core = axis_split(r, c)

    def col_of(yh_, z_, core_):
        return yh_ * 8 + (z_ % 4) * 2 + core_

    def row_of(x_, yl_):
        return (x_ % 4) * 2 + yl_

    open_sends = []

    def send(src, dst, ss, rs, to):
        copy = pltpu.make_async_remote_copy(
            src_ref=src, dst_ref=dst, send_sem=ss, recv_sem=rs, device_id=to,
            device_id_type=pl.DeviceIdType.MESH,
        )
        copy.start()
        open_sends.append(copy)

    def arrived(ref, sem):
        pltpu.make_async_copy(ref, ref, sem).wait()

    own = [
        pltpu.make_async_copy(stored.at[pl.ds(2 * r, 2)], zs.at[c, r], own_sem.at[0]),
        pltpu.make_async_copy(stored.at[c], xs.at[r, c], own_sem.at[1]),
        pltpu.make_async_copy(stored.at[0], cp.at[core, r], own_sem.at[2]),
    ]
    for copy in own:
        copy.start()
    for d in range(1, 8):
        to = (r + d) % 8
        send(panels.at[pl.ds(2 * to, 2)], zs.at[c, r], p1a.at[d], p1a_got.at[d], (to, c))
    for d in range(1, 16):
        to = (c + d) % 16
        send(panels.at[to], xs.at[r, c], p1x.at[d], p1x_got.at[d], (r, to))
    for d in range(1, 8):
        send(panels.at[0], cp.at[core, r], p1c.at[d], p1c_got.at[d], ((r + d) % 8, c))

    def h_tile(i, j):
        rows = pl.ds(pl.multiple_of(i * 128, 128), 128)
        return h_ref.at[rows, pl.ds(pl.multiple_of(j * 128, 128), 128)]

    def send_tile(n, carry):
        m = n * (37 + 54 * core) % 128
        i = row_of(x + m % 4, (yl + m // 4) % 2)
        j = col_of((2 * yh + yl + m // 4) // 2 % 2, z + m // 16, (core + m // 64) % 2)
        pltpu.make_async_remote_copy(
            src_ref=h_tile(i, j), dst_ref=near.at[r * 16 + c], send_sem=h_sent, recv_sem=h_got,
            device_id=(i, j), device_id_type=pl.DeviceIdType.MESH,
        ).start()
        return carry

    lax.fori_loop(1, EARLY, send_tile, 0)

    zp, zm = (r, col_of(yh, z + 1, core)), (r, col_of(yh, z + 3, core))
    yp, sib = (r, col_of(1 - yh, z, core)), (r, col_of(yh, z, 1 - core))
    xp, xm, lp = (row_of(x + 1, yl), c), (row_of(x + 3, yl), c), (row_of(x, 1 - yl), c)

    def ring(ref, base, index, side, ahead, behind):
        half = ref.shape[1] // 2
        first = lambda k: ref.at[k, pl.ds(0, half)]
        second = lambda k: ref.at[k, pl.ds(half, half)]

        def out(piece, i, to):
            send(piece, piece, sends.at[base + i], gets.at[base + i], to)

        def start():
            mine = index(0, 0)
            out(ref.at[mine], 0, side)
            out(ref.at[mine], 1, ahead)
            out(ref.at[mine], 2, behind)

        def onward(plane):
            i = 1 + 4 * plane
            arrived(ref.at[index(plane, 3)], gets.at[base + i])
            out(first(index(plane, 3)), i + 2, ahead)
            arrived(ref.at[index(plane, 1)], gets.at[base + i + 1])
            out(second(index(plane, 1)), i + 3, behind)

        def beside():
            other = index(1, 0)
            arrived(ref.at[other], gets.at[base])
            out(ref.at[other], 5, ahead)
            out(ref.at[other], 6, behind)

        def last(plane):
            i = 3 + 4 * plane
            arrived(first(index(plane, 2)), gets.at[base + i])
            arrived(second(index(plane, 2)), gets.at[base + i + 1])

        return start, onward, beside, last

    def col_index(plane, d):
        return col_of(yh if plane == 0 else 1 - yh, z + d, core)

    def row_index(plane, d):
        return row_of(x + d, yl if plane == 0 else 1 - yl)

    start_a, onward_a, beside_a, last_a = ring(zs, 0, col_index, yp, zp, zm)
    start_x, onward_x, beside_x, last_x = ring(xs, 9, row_index, lp, xp, xm)
    start_c, onward_c, beside_c, last_c = ring(cs, 18, col_index, yp, zp, zm)
    shares = [(0, 0), (0, 3), (0, 1), (1, 0), (1, 3), (1, 1), (0, 2), (1, 2)]

    def share(ref, ss, rs, i):
        piece = ref.at[col_index(*shares[i])]
        send(piece, piece, ss.at[i], rs.at[i], sib)

    def shared(ref, rs, i):
        plane, d = shares[i]
        arrived(ref.at[col_of(yh if plane == 0 else 1 - yh, z + d, 1 - core)], rs.at[i])

    own[0].wait()
    for d in range(1, 8):
        arrived(zs.at[c, (r + 8 - d) % 8], p1a_got.at[d])
    start_a()
    own[1].wait()
    for d in range(1, 16):
        arrived(xs.at[r, (c + 16 - d) % 16], p1x_got.at[d])
    start_x()
    own[2].wait()
    for d in range(1, 8):
        arrived(cp.at[core, (r + 8 - d) % 8], p1c_got.at[d])
    send(cp.at[core], cp.at[core], p1c.at[0], p1c_got.at[0], sib)
    arrived(cp.at[1 - core], p1c_got.at[0])
    for i in range(4):
        p = row_owner[4 * core + i]
        cs[c, i] = cp[p % 2, p // 2]
    share(zs, sib_a, sib_a_got, 0)
    start_c()
    share(cs, sib_c, sib_c_got, 0)
    onward_x(0)
    onward_a(0)
    beside_x()
    beside_a()
    onward_c(0)
    beside_c()
    for i in range(1, 4):
        share(zs, sib_a, sib_a_got, i)
        share(cs, sib_c, sib_c_got, i)
    onward_x(1)
    onward_a(1)
    onward_c(1)
    for i in range(4, 6):
        share(cs, sib_c, sib_c_got, i)
        share(zs, sib_a, sib_a_got, i)
    last_a(0)
    share(zs, sib_a, sib_a_got, 6)
    last_c(0)
    share(cs, sib_c, sib_c_got, 6)
    last_c(1)
    share(cs, sib_c, sib_c_got, 7)
    for i in range(8):
        shared(cs, sib_c_got, i)

    last_a(1)
    share(zs, sib_a, sib_a_got, 7)
    for plane in range(2):
        last_x(plane)
    for i in range(8):
        shared(zs, sib_a_got, i)
    lax.fori_loop(EARLY, 128, send_tile, 0)
    kept = pltpu.make_async_copy(h_tile(r, c), near.at[r * 16 + c], h_got)
    kept.start()
    fetch_panel(
        lambda i, p, q: cs[2 * q + i // 4, i % 4],
        PANEL // BLOCK, 0, row_owner, col_owner, s_buf, corner_h,
    )
    corner_inverse(s_buf, work, a_blk, b_blk, inv)

    def strip_step(t, carry):
        fetch_panel(
            lambda i, p, q: xs[p // 2, 2 * q + p % 2],
            TALL // BLOCK, c * 16 + t * 4, row_owner, col_owner, s_buf, h_buf,
        )
        special = jnp.logical_and(c == 0, t < 2)
        _, coupling = coupling_of(s_buf[:TALL, :], inv, special, t)
        rest = h_buf[...] - dot(coupling, corner_h[...], 1, 0, HIGHEST)
        at = pl.ds(pl.multiple_of(t * TALL, TALL), TALL)
        rh[at, :PANEL], rl[at, :PANEL] = halves(rest)
        rh[at, PANEL:], rl[at, PANEL:] = halves(coupling)
        return carry

    lax.fori_loop(0, rh.shape[0] // TALL, strip_step, 0)

    def rows_of(t):
        return pl.ds(pl.multiple_of(t * TALL, TALL), TALL)

    def band_step(t, carry):
        slot = t // 4
        fetch_panel(
            lambda i, p, q: zs[2 * q + p % 2, p // 2, slot],
            TALL // BLOCK, r * 32 + t * 4, row_owner, col_owner, s_buf, h_buf,
        )
        special = jnp.logical_and(r == 0, t < 2)
        panel, coupling = coupling_of(s_buf[:TALL, :], inv, special, t)
        f_buf[rows_of(t), :] = panel
        lh[:, :PANEL], ll[:, :PANEL] = halves(coupling)
        lh[:, PANEL:], ll[:, PANEL:] = halves(h_buf[...])
        total = dot(lh[...], rh[...], 1, 1)
        total = total + dot(lh[...], rl[...], 1, 1)
        u_buf[rows_of(t), :] = total + dot(ll[...], rh[...], 1, 1)
        pltpu.make_async_copy(u_buf.at[rows_of(t)], update.at[rows_of(t)], out_sem.at[0, t]).start()
        pltpu.make_async_copy(f_buf.at[rows_of(t)], factor.at[rows_of(t)], out_sem.at[1, t]).start()
        return carry

    steps = u_buf.shape[0] // TALL
    lax.fori_loop(0, steps, band_step, 0)
    for t in range(steps):
        pltpu.make_async_copy(u_buf.at[rows_of(t)], update.at[rows_of(t)], out_sem.at[0, t]).wait()
        pltpu.make_async_copy(f_buf.at[rows_of(t)], factor.at[rows_of(t)], out_sem.at[1, t]).wait()
    arrived(near, h_got)
    arrived(near.at[pl.ds(0, 127)], h_sent)
    for copy in open_sends:
        copy.wait_send()


SMEM = pl.BlockSpec(memory_space=pltpu.SMEM)


def shape_of(shape, dtype=F32):
    return jax.ShapeDtypeStruct(shape, dtype)


def per_device(h_old, s_old, row_owner, col_owner):
    rows_n = lax.axis_size("row")
    cols_n = lax.axis_size("col")
    row_id = lax.axis_index("row")
    col_id = lax.axis_index("col")
    place = jnp.stack([row_id, col_id]).astype(jnp.int32)
    local_h = h_old[0, 0]
    local_s = s_old[0, 0]
    band = ORDER // rows_n
    strip = ORDER // cols_n
    panels = jnp.concatenate([local_s, local_h[:, :BLOCK]], axis=1).reshape(16, BLOCK, 128)
    any_space = pl.BlockSpec(memory_space=pl.ANY)
    dma = pltpu.SemaphoreType.DMA
    vmem = pltpu.VMEM
    near, update, factor = pl.pallas_call(
        panel_kernel,
        out_shape=(shape_of((128, 128, 128)), shape_of((band, strip)), shape_of((band, PANEL))),
        in_specs=[pl.BlockSpec(memory_space=pltpu.VMEM), any_space, any_space, SMEM, SMEM],
        out_specs=(any_space,) * 3,
        scratch_shapes=[
            vmem((16, 8, 2, BLOCK, 128), F32),
            vmem((16, 4, BLOCK, 128), F32),
            vmem((2, 8, BLOCK, 128), F32),
            vmem((8, 16, BLOCK, 128), F32),
            vmem((PANEL // STEP, STEP, 2 * PANEL), F32),
            vmem((STEP, STEP), F32),
            vmem((STEP, STEP), F32),
            vmem((PANEL, PANEL), F32),
            vmem((PANEL, PANEL), F32),
            vmem((PANEL, PANEL), F32),
            vmem((TALL, PANEL), F32),
            vmem((strip, 2 * PANEL), BF16),
            vmem((strip, 2 * PANEL), BF16),
            vmem((TALL, 2 * PANEL), BF16),
            vmem((TALL, 2 * PANEL), BF16),
            vmem((band, PANEL), F32),
            vmem((band, strip), F32),
            dma((3,)), dma((8,)), dma((8,)), dma((16,)), dma((16,)), dma((8,)), dma((8,)),
            dma((27,)), dma((27,)), dma((8,)), dma((8,)), dma((8,)), dma((8,)), dma, dma,
            dma((2, band // TALL)),
        ],
        compiler_params=pltpu.CompilerParams(has_side_effects=True, vmem_limit_bytes=60 * 2**20),
        cost_estimate=pl.CostEstimate(flops=4 * 10**10, bytes_accessed=64 * 2**20, transcendentals=0),
        name="panel",
    )(panels, panels, local_h, row_owner, col_owner)
    h_tiles = near.reshape(rows_n, cols_n, 128, 128)

    fine = pl.BlockSpec((16, 1, FINE, strip), lambda s, u: (s, u, 0, 0))
    h_block = pl.pallas_call(
        final_kernel,
        grid=(2, BLOCK // FINE),
        out_shape=shape_of((band // BLOCK, BLOCK // FINE, FINE, strip)),
        in_specs=[
            SMEM, SMEM, SMEM,
            pl.BlockSpec((rows_n, cols_n, FINE, 128), lambda s, u: (0, 0, s * (BLOCK // FINE) + u, 0)),
            fine,
        ],
        out_specs=fine,
        compiler_params=pltpu.CompilerParams(vmem_limit_bytes=60 * 2**20),
        cost_estimate=pl.CostEstimate(flops=2**22, bytes_accessed=24 * 2**20, transcendentals=0),
        name="final",
    )(place, row_owner, col_owner, h_tiles, update.reshape(band // BLOCK, BLOCK // FINE, FINE, strip))
    return h_block.reshape(band, strip), factor


def solution(mesh):
    in_specs = (P("row", "col", None, None), P("row", "col", None, None), P(), P())
    out_specs = (P("row", "col"), P("row", None))
    return jax.shard_map(
        per_device, mesh=mesh, in_specs=in_specs, out_specs=out_specs, check_vma=False
    )
```

```python
import jax
import jax.numpy as jnp
from jax import lax
from jax.experimental import pallas as pl
from jax.experimental.pallas import tpu as pltpu
from jax.sharding import PartitionSpec as P

ORDER = 16384
PANEL = 512
BLOCK = 64
STEP = 128
FINE = 32
TALL = 256
EARLY = 1
HIGHEST = lax.Precision.HIGHEST
BF16 = jnp.bfloat16
F32 = jnp.float32


def dot(a, b, ca, cb, precision=None):
    return lax.dot_general(
        a, b, (((ca,), (cb,)), ((), ())), precision=precision, preferred_element_type=F32
    )


def halves(x):
    high = x.astype(BF16)
    return high, (x - high.astype(F32)).astype(BF16)


def lower_half(shape):
    return lax.broadcasted_iota(jnp.int32, shape, 1) < BLOCK


def fetch_panel(read, rows, first, row_owner, col_owner, s_out, h_out):
    low = lower_half((BLOCK, 2 * BLOCK))
    for i in range(rows):
        p = row_owner[first + i]
        for k in range(0, PANEL // BLOCK, 2):
            one = read(i, p, col_owner[k])
            two = read(i, p, col_owner[k + 1])
            at = (pl.ds(i * BLOCK, BLOCK), pl.ds(k * BLOCK, 2 * BLOCK))
            s_out[at] = jnp.where(low, one, pltpu.roll(two, BLOCK, 1))
            h_out[at] = jnp.where(low, pltpu.roll(one, BLOCK, 1), two)


def spread(x, rows):
    return jnp.broadcast_to(x, (rows, x.shape[1]))


def factor_inverse(a_ref, b_ref):
    sub = lax.broadcasted_iota(jnp.int32, (8, STEP), 0)
    for j in range(0, STEP, 8):
        far = STEP - j - 8
        a_near, b_near = a_ref[j : j + 8, :], b_ref[j : j + 8, :]
        near = [jnp.broadcast_to(a_near[:, j + t : j + t + 1], (8, STEP)) for t in range(8)]
        if far:
            a_far, b_far = a_ref[j + 8 :, :], b_ref[j + 8 :, :]
            cols = [jnp.broadcast_to(a_far[:, j + t : j + t + 1], (far, STEP)) for t in range(8)]
        scales, links = [], []
        for t in range(8):
            r = lax.rsqrt(near[t][t : t + 1, :])
            l = near[t] * spread(r, 8)
            below = jnp.where(sub > t, l, 0.0)
            a_row, b_row = a_near[t : t + 1, :] * r, b_near[t : t + 1, :] * r
            a_near = jnp.where(sub == t, spread(a_row, 8), a_near - below * spread(a_row, 8))
            b_near = jnp.where(sub == t, spread(b_row, 8), b_near - below * spread(b_row, 8))
            link = {}
            for u in range(t + 1, 8):
                link[u] = l[u : u + 1, :]
                near[u] = near[u] - l * spread(link[u], 8)
            scales.append(r)
            links.append(link)
        b_ref[j : j + 8, :] = b_near
        if far:
            for t in range(8):
                l = cols[t] * spread(scales[t], far)
                for u in range(t + 1, 8):
                    cols[u] = cols[u] - l * spread(links[t][u], far)
                a_far = a_far - l * spread(a_near[t : t + 1, :], far)
                b_far = b_far - l * spread(b_near[t : t + 1, :], far)
            a_ref[j + 8 :, :] = a_far
            b_ref[j + 8 :, :] = b_far


def corner_inverse(s_top, work, a_blk, b_blk, inverse):
    eye = lax.broadcasted_iota(jnp.int32, (STEP, STEP), 0) == lax.broadcasted_iota(
        jnp.int32, (STEP, STEP), 1
    )
    eye = jnp.where(eye, 1.0, 0.0)
    count = PANEL // STEP
    for k in range(count):
        work[k, :, :PANEL] = s_top[k * STEP : (k + 1) * STEP, :]
        work[k, :, PANEL:] = jnp.zeros((STEP, PANEL), F32)
        work[k, :, PANEL + k * STEP : PANEL + (k + 1) * STEP] = eye
    lane = lax.broadcasted_iota(jnp.int32, (STEP, PANEL), 1)

    def step(k, carry):
        a_blk[...] = work[k, :, pl.ds(pl.multiple_of(k * STEP, STEP), STEP)]
        b_blk[...] = eye
        factor_inverse(a_blk, b_blk)
        rows = dot(b_blk[...], work[k], 1, 0, HIGHEST)
        work[k] = rows
        ahead = jnp.where(lane >= (k + 1) * STEP, rows[:, :PANEL], 0.0).T
        for i in range(1, count):
            work[i] = work[i] - dot(ahead[i * STEP : (i + 1) * STEP], rows, 1, 0, HIGHEST)
        return carry

    lax.fori_loop(0, count, step, 0)
    for k in range(count):
        inverse[k * STEP : (k + 1) * STEP, :] = work[k, :, PANEL:]


def coupling_of(s_rows, inv, special, step):
    inverse = inv[...]
    factor = dot(s_rows, inverse, 1, 1, HIGHEST)
    coupling = dot(factor, inverse, 1, 0, HIGHEST)
    at = pl.multiple_of(lax.rem(step, 2) * TALL, TALL)
    shape = (TALL, PANEL)
    eye = at + lax.broadcasted_iota(jnp.int32, shape, 0) == lax.broadcasted_iota(jnp.int32, shape, 1)
    top = jnp.where(eye, 1.0, 0.0) - inv[pl.ds(at, TALL), :]
    return factor, jnp.where(special, top, coupling)


def final_kernel(place, row_owner, col_owner, tiles, update, out):
    slot = pl.program_id(0)
    low = lower_half((FINE, 2 * BLOCK))
    owners = [col_owner[place[1] * 16 + j] * 2 for j in range(16)]
    for i in range(16):
        p = row_owner[place[0] * 32 + slot * 16 + i]
        for j in range(0, 16, 2):
            one = tiles[p // 2, owners[j] + p % 2]
            two = tiles[p // 2, owners[j + 1] + p % 2]
            if j < 8:
                both = jnp.where(low, one, pltpu.roll(two, BLOCK, 1))
            else:
                both = jnp.where(low, pltpu.roll(one, BLOCK, 1), two)
            at = (i, 0, slice(None), pl.ds(j * BLOCK, 2 * BLOCK))
            out[at] = both - update[at]


def axis_split(r, c):
    return r // 2, r % 2, c // 8, (c // 2) % 4, c % 2


def panel_kernel(panels, stored, h_ref, row_owner, col_owner, near, update, factor,
                 zs, cs, cp, xs, work, a_blk, b_blk, inv, corner_h, s_buf, h_buf,
                 rh, rl, lh, ll, f_buf, u_buf,
                 own_sem, p1a, p1a_got, p1x, p1x_got, p1c, p1c_got, sends, gets,
                 sib_a, sib_a_got, sib_c, sib_c_got, h_sent, h_got, out_sem):
    r, c = lax.axis_index("row"), lax.axis_index("col")
    x, yl, yh, z, core = axis_split(r, c)

    def col_of(yh_, z_, core_):
        return yh_ * 8 + (z_ % 4) * 2 + core_

    def row_of(x_, yl_):
        return (x_ % 4) * 2 + yl_

    open_sends = []

    def send(src, dst, ss, rs, to):
        copy = pltpu.make_async_remote_copy(
            src_ref=src, dst_ref=dst, send_sem=ss, recv_sem=rs, device_id=to,
            device_id_type=pl.DeviceIdType.MESH,
        )
        copy.start()
        open_sends.append(copy)

    def arrived(ref, sem):
        pltpu.make_async_copy(ref, ref, sem).wait()

    own = [
        pltpu.make_async_copy(stored.at[pl.ds(2 * r, 2)], zs.at[c, r], own_sem.at[0]),
        pltpu.make_async_copy(stored.at[c], xs.at[r, c], own_sem.at[1]),
        pltpu.make_async_copy(stored.at[0], cp.at[core, r], own_sem.at[2]),
    ]
    for copy in own:
        copy.start()
    for d in range(1, 8):
        to = (r + d) % 8
        send(panels.at[pl.ds(2 * to, 2)], zs.at[c, r], p1a.at[d], p1a_got.at[d], (to, c))
    for d in range(1, 16):
        to = (c + d) % 16
        send(panels.at[to], xs.at[r, c], p1x.at[d], p1x_got.at[d], (r, to))
    for d in range(1, 8):
        send(panels.at[0], cp.at[core, r], p1c.at[d], p1c_got.at[d], ((r + d) % 8, c))

    def h_tile(i, j):
        rows = pl.ds(pl.multiple_of(i * 128, 128), 128)
        return h_ref.at[rows, pl.ds(pl.multiple_of(j * 128, 128), 128)]

    def send_tile(n, carry):
        m = n * (37 + 54 * core) % 128
        i = row_of(x + m % 4, (yl + m // 4) % 2)
        j = col_of((2 * yh + yl + m // 4) // 2 % 2, z + m // 16, (core + m // 64) % 2)
        pltpu.make_async_remote_copy(
            src_ref=h_tile(i, j), dst_ref=near.at[r * 16 + c], send_sem=h_sent, recv_sem=h_got,
            device_id=(i, j), device_id_type=pl.DeviceIdType.MESH,
        ).start()
        return carry

    lax.fori_loop(1, EARLY, send_tile, 0)

    zp, zm = (r, col_of(yh, z + 1, core)), (r, col_of(yh, z + 3, core))
    yp, sib = (r, col_of(1 - yh, z, core)), (r, col_of(yh, z, 1 - core))
    xp, xm, lp = (row_of(x + 1, yl), c), (row_of(x + 3, yl), c), (row_of(x, 1 - yl), c)

    def ring(ref, base, index, side, ahead, behind):
        half = ref.shape[1] // 2
        first = lambda k: ref.at[k, pl.ds(0, half)]
        second = lambda k: ref.at[k, pl.ds(half, half)]

        def out(piece, i, to):
            send(piece, piece, sends.at[base + i], gets.at[base + i], to)

        def start():
            mine = index(0, 0)
            out(ref.at[mine], 0, side)
            out(ref.at[mine], 1, ahead)
            out(ref.at[mine], 2, behind)

        def onward(plane):
            i = 1 + 4 * plane
            arrived(ref.at[index(plane, 3)], gets.at[base + i])
            out(first(index(plane, 3)), i + 2, ahead)
            arrived(ref.at[index(plane, 1)], gets.at[base + i + 1])
            out(second(index(plane, 1)), i + 3, behind)

        def beside():
            other = index(1, 0)
            arrived(ref.at[other], gets.at[base])
            out(ref.at[other], 5, ahead)
            out(ref.at[other], 6, behind)

        def last(plane):
            i = 3 + 4 * plane
            arrived(first(index(plane, 2)), gets.at[base + i])
            arrived(second(index(plane, 2)), gets.at[base + i + 1])

        return start, onward, beside, last

    def col_index(plane, d):
        return col_of(yh if plane == 0 else 1 - yh, z + d, core)

    def row_index(plane, d):
        return row_of(x + d, yl if plane == 0 else 1 - yl)

    start_a, onward_a, beside_a, last_a = ring(zs, 0, col_index, yp, zp, zm)
    start_x, onward_x, beside_x, last_x = ring(xs, 9, row_index, lp, xp, xm)
    start_c, onward_c, beside_c, last_c = ring(cs, 18, col_index, yp, zp, zm)
    shares = [(0, 0), (0, 3), (0, 1), (1, 0), (1, 3), (1, 1), (0, 2), (1, 2)]

    def share(ref, ss, rs, i):
        piece = ref.at[col_index(*shares[i])]
        send(piece, piece, ss.at[i], rs.at[i], sib)

    def shared(ref, rs, i):
        plane, d = shares[i]
        arrived(ref.at[col_of(yh if plane == 0 else 1 - yh, z + d, 1 - core)], rs.at[i])

    own[0].wait()
    for d in range(1, 8):
        arrived(zs.at[c, (r + 8 - d) % 8], p1a_got.at[d])
    start_a()
    own[1].wait()
    for d in range(1, 16):
        arrived(xs.at[r, (c + 16 - d) % 16], p1x_got.at[d])
    start_x()
    own[2].wait()
    for d in range(1, 8):
        arrived(cp.at[core, (r + 8 - d) % 8], p1c_got.at[d])
    send(cp.at[core], cp.at[core], p1c.at[0], p1c_got.at[0], sib)
    arrived(cp.at[1 - core], p1c_got.at[0])
    for i in range(4):
        p = row_owner[4 * core + i]
        cs[c, i] = cp[p % 2, p // 2]
    share(zs, sib_a, sib_a_got, 0)
    start_c()
    share(cs, sib_c, sib_c_got, 0)
    onward_a(0)
    onward_x(0)
    beside_a()
    beside_x()
    onward_c(0)
    beside_c()
    for i in range(1, 4):
        share(zs, sib_a, sib_a_got, i)
        share(cs, sib_c, sib_c_got, i)
    onward_a(1)
    onward_x(1)
    onward_c(1)
    for i in range(4, 6):
        share(cs, sib_c, sib_c_got, i)
        share(zs, sib_a, sib_a_got, i)
    last_a(0)
    share(zs, sib_a, sib_a_got, 6)
    last_c(0)
    share(cs, sib_c, sib_c_got, 6)
    last_c(1)
    share(cs, sib_c, sib_c_got, 7)
    last_a(1)
    share(zs, sib_a, sib_a_got, 7)
    lax.fori_loop(EARLY, 128, send_tile, 0)
    kept = pltpu.make_async_copy(h_tile(r, c), near.at[r * 16 + c], h_got)
    kept.start()
    for plane in range(2):
        last_x(plane)
    for i in range(8):
        shared(cs, sib_c_got, i)
    for i in range(8):
        shared(zs, sib_a_got, i)

    fetch_panel(
        lambda i, p, q: cs[2 * q + i // 4, i % 4],
        PANEL // BLOCK, 0, row_owner, col_owner, s_buf, corner_h,
    )
    corner_inverse(s_buf, work, a_blk, b_blk, inv)

    def strip_step(t, carry):
        fetch_panel(
            lambda i, p, q: xs[p // 2, 2 * q + p % 2],
            TALL // BLOCK, c * 16 + t * 4, row_owner, col_owner, s_buf, h_buf,
        )
        special = jnp.logical_and(c == 0, t < 2)
        _, coupling = coupling_of(s_buf[:TALL, :], inv, special, t)
        rest = h_buf[...] - dot(coupling, corner_h[...], 1, 0, HIGHEST)
        at = pl.ds(pl.multiple_of(t * TALL, TALL), TALL)
        rh[at, :PANEL], rl[at, :PANEL] = halves(rest)
        rh[at, PANEL:], rl[at, PANEL:] = halves(coupling)
        return carry

    lax.fori_loop(0, rh.shape[0] // TALL, strip_step, 0)

    def rows_of(t):
        return pl.ds(pl.multiple_of(t * TALL, TALL), TALL)

    def band_step(t, carry):
        slot = t // 4
        fetch_panel(
            lambda i, p, q: zs[2 * q + p % 2, p // 2, slot],
            TALL // BLOCK, r * 32 + t * 4, row_owner, col_owner, s_buf, h_buf,
        )
        special = jnp.logical_and(r == 0, t < 2)
        panel, coupling = coupling_of(s_buf[:TALL, :], inv, special, t)
        f_buf[rows_of(t), :] = panel
        lh[:, :PANEL], ll[:, :PANEL] = halves(coupling)
        lh[:, PANEL:], ll[:, PANEL:] = halves(h_buf[...])
        total = dot(lh[...], rh[...], 1, 1)
        total = total + dot(lh[...], rl[...], 1, 1)
        u_buf[rows_of(t), :] = total + dot(ll[...], rh[...], 1, 1)
        pltpu.make_async_copy(u_buf.at[rows_of(t)], update.at[rows_of(t)], out_sem.at[0, t]).start()
        pltpu.make_async_copy(f_buf.at[rows_of(t)], factor.at[rows_of(t)], out_sem.at[1, t]).start()
        return carry

    steps = u_buf.shape[0] // TALL
    lax.fori_loop(0, steps, band_step, 0)
    for t in range(steps):
        pltpu.make_async_copy(u_buf.at[rows_of(t)], update.at[rows_of(t)], out_sem.at[0, t]).wait()
        pltpu.make_async_copy(f_buf.at[rows_of(t)], factor.at[rows_of(t)], out_sem.at[1, t]).wait()
    arrived(near, h_got)
    arrived(near.at[pl.ds(0, 127)], h_sent)
    for copy in open_sends:
        copy.wait_send()


SMEM = pl.BlockSpec(memory_space=pltpu.SMEM)


def shape_of(shape, dtype=F32):
    return jax.ShapeDtypeStruct(shape, dtype)


def per_device(h_old, s_old, row_owner, col_owner):
    rows_n = lax.axis_size("row")
    cols_n = lax.axis_size("col")
    row_id = lax.axis_index("row")
    col_id = lax.axis_index("col")
    place = jnp.stack([row_id, col_id]).astype(jnp.int32)
    local_h = h_old[0, 0]
    local_s = s_old[0, 0]
    band = ORDER // rows_n
    strip = ORDER // cols_n
    panels = jnp.concatenate([local_s, local_h[:, :BLOCK]], axis=1).reshape(16, BLOCK, 128)
    any_space = pl.BlockSpec(memory_space=pl.ANY)
    dma = pltpu.SemaphoreType.DMA
    vmem = pltpu.VMEM
    near, update, factor = pl.pallas_call(
        panel_kernel,
        out_shape=(shape_of((128, 128, 128)), shape_of((band, strip)), shape_of((band, PANEL))),
        in_specs=[pl.BlockSpec(memory_space=pltpu.VMEM), any_space, any_space, SMEM, SMEM],
        out_specs=(any_space,) * 3,
        scratch_shapes=[
            vmem((16, 8, 2, BLOCK, 128), F32),
            vmem((16, 4, BLOCK, 128), F32),
            vmem((2, 8, BLOCK, 128), F32),
            vmem((8, 16, BLOCK, 128), F32),
            vmem((PANEL // STEP, STEP, 2 * PANEL), F32),
            vmem((STEP, STEP), F32),
            vmem((STEP, STEP), F32),
            vmem((PANEL, PANEL), F32),
            vmem((PANEL, PANEL), F32),
            vmem((PANEL, PANEL), F32),
            vmem((TALL, PANEL), F32),
            vmem((strip, 2 * PANEL), BF16),
            vmem((strip, 2 * PANEL), BF16),
            vmem((TALL, 2 * PANEL), BF16),
            vmem((TALL, 2 * PANEL), BF16),
            vmem((band, PANEL), F32),
            vmem((band, strip), F32),
            dma((3,)), dma((8,)), dma((8,)), dma((16,)), dma((16,)), dma((8,)), dma((8,)),
            dma((27,)), dma((27,)), dma((8,)), dma((8,)), dma((8,)), dma((8,)), dma, dma,
            dma((2, band // TALL)),
        ],
        compiler_params=pltpu.CompilerParams(has_side_effects=True, vmem_limit_bytes=60 * 2**20),
        cost_estimate=pl.CostEstimate(flops=4 * 10**10, bytes_accessed=64 * 2**20, transcendentals=0),
        name="panel",
    )(panels, panels, local_h, row_owner, col_owner)
    h_tiles = near.reshape(rows_n, cols_n, 128, 128)

    fine = pl.BlockSpec((16, 1, FINE, strip), lambda s, u: (s, u, 0, 0))
    h_block = pl.pallas_call(
        final_kernel,
        grid=(2, BLOCK // FINE),
        out_shape=shape_of((band // BLOCK, BLOCK // FINE, FINE, strip)),
        in_specs=[
            SMEM, SMEM, SMEM,
            pl.BlockSpec((rows_n, cols_n, FINE, 128), lambda s, u: (0, 0, s * (BLOCK // FINE) + u, 0)),
            fine,
        ],
        out_specs=fine,
        compiler_params=pltpu.CompilerParams(vmem_limit_bytes=60 * 2**20),
        cost_estimate=pl.CostEstimate(flops=2**22, bytes_accessed=24 * 2**20, transcendentals=0),
        name="final",
    )(place, row_owner, col_owner, h_tiles, update.reshape(band // BLOCK, BLOCK // FINE, FINE, strip))
    return h_block.reshape(band, strip), factor


def solution(mesh):
    in_specs = (P("row", "col", None, None), P("row", "col", None, None), P(), P())
    out_specs = (P("row", "col"), P("row", None))
    return jax.shard_map(
        per_device, mesh=mesh, in_specs=in_specs, out_specs=out_specs, check_vma=False
    )
```

```python
import jax
import jax.numpy as jnp
from jax import lax
from jax.experimental import pallas as pl
from jax.experimental.pallas import tpu as pltpu
from jax.sharding import PartitionSpec as P

ORDER = 16384
PANEL = 512
BLOCK = 64
STEP = 128
FINE = 32
TALL = 256
EARLY = 1
HIGHEST = lax.Precision.HIGHEST
BF16 = jnp.bfloat16
F32 = jnp.float32


def dot(a, b, ca, cb, precision=None):
    return lax.dot_general(
        a, b, (((ca,), (cb,)), ((), ())), precision=precision, preferred_element_type=F32
    )


def halves(x):
    high = x.astype(BF16)
    return high, (x - high.astype(F32)).astype(BF16)


def lower_half(shape):
    return lax.broadcasted_iota(jnp.int32, shape, 1) < BLOCK


def fetch_panel(read, rows, first, row_owner, col_owner, s_out, h_out):
    low = lower_half((BLOCK, 2 * BLOCK))
    for i in range(rows):
        p = row_owner[first + i]
        for k in range(0, PANEL // BLOCK, 2):
            one = read(i, p, col_owner[k])
            two = read(i, p, col_owner[k + 1])
            at = (pl.ds(i * BLOCK, BLOCK), pl.ds(k * BLOCK, 2 * BLOCK))
            s_out[at] = jnp.where(low, one, pltpu.roll(two, BLOCK, 1))
            h_out[at] = jnp.where(low, pltpu.roll(one, BLOCK, 1), two)


def spread(x, rows):
    return jnp.broadcast_to(x, (rows, x.shape[1]))


def factor_inverse(a_ref, b_ref):
    sub = lax.broadcasted_iota(jnp.int32, (8, STEP), 0)
    for j in range(0, STEP, 8):
        far = STEP - j - 8
        a_near, b_near = a_ref[j : j + 8, :], b_ref[j : j + 8, :]
        near = [jnp.broadcast_to(a_near[:, j + t : j + t + 1], (8, STEP)) for t in range(8)]
        if far:
            a_far, b_far = a_ref[j + 8 :, :], b_ref[j + 8 :, :]
            cols = [jnp.broadcast_to(a_far[:, j + t : j + t + 1], (far, STEP)) for t in range(8)]
        scales, links = [], []
        for t in range(8):
            r = lax.rsqrt(near[t][t : t + 1, :])
            l = near[t] * spread(r, 8)
            below = jnp.where(sub > t, l, 0.0)
            a_row, b_row = a_near[t : t + 1, :] * r, b_near[t : t + 1, :] * r
            a_near = jnp.where(sub == t, spread(a_row, 8), a_near - below * spread(a_row, 8))
            b_near = jnp.where(sub == t, spread(b_row, 8), b_near - below * spread(b_row, 8))
            link = {}
            for u in range(t + 1, 8):
                link[u] = l[u : u + 1, :]
                near[u] = near[u] - l * spread(link[u], 8)
            scales.append(r)
            links.append(link)
        b_ref[j : j + 8, :] = b_near
        if far:
            for t in range(8):
                l = cols[t] * spread(scales[t], far)
                for u in range(t + 1, 8):
                    cols[u] = cols[u] - l * spread(links[t][u], far)
                a_far = a_far - l * spread(a_near[t : t + 1, :], far)
                b_far = b_far - l * spread(b_near[t : t + 1, :], far)
            a_ref[j + 8 :, :] = a_far
            b_ref[j + 8 :, :] = b_far


def corner_inverse(s_top, work, a_blk, b_blk, inverse):
    eye = lax.broadcasted_iota(jnp.int32, (STEP, STEP), 0) == lax.broadcasted_iota(
        jnp.int32, (STEP, STEP), 1
    )
    eye = jnp.where(eye, 1.0, 0.0)
    count = PANEL // STEP
    for k in range(count):
        work[k, :, :PANEL] = s_top[k * STEP : (k + 1) * STEP, :]
        work[k, :, PANEL:] = jnp.zeros((STEP, PANEL), F32)
        work[k, :, PANEL + k * STEP : PANEL + (k + 1) * STEP] = eye
    lane = lax.broadcasted_iota(jnp.int32, (STEP, PANEL), 1)

    def step(k, carry):
        a_blk[...] = work[k, :, pl.ds(pl.multiple_of(k * STEP, STEP), STEP)]
        b_blk[...] = eye
        factor_inverse(a_blk, b_blk)
        rows = dot(b_blk[...], work[k], 1, 0, HIGHEST)
        work[k] = rows
        ahead = jnp.where(lane >= (k + 1) * STEP, rows[:, :PANEL], 0.0).T
        for i in range(1, count):
            work[i] = work[i] - dot(ahead[i * STEP : (i + 1) * STEP], rows, 1, 0, HIGHEST)
        return carry

    lax.fori_loop(0, count, step, 0)
    for k in range(count):
        inverse[k * STEP : (k + 1) * STEP, :] = work[k, :, PANEL:]


def coupling_of(s_rows, inv, special, step):
    inverse = inv[...]
    factor = dot(s_rows, inverse, 1, 1, HIGHEST)
    coupling = dot(factor, inverse, 1, 0, HIGHEST)
    at = pl.multiple_of(lax.rem(step, 2) * TALL, TALL)
    shape = (TALL, PANEL)
    eye = at + lax.broadcasted_iota(jnp.int32, shape, 0) == lax.broadcasted_iota(jnp.int32, shape, 1)
    top = jnp.where(eye, 1.0, 0.0) - inv[pl.ds(at, TALL), :]
    return factor, jnp.where(special, top, coupling)


def final_kernel(place, row_owner, col_owner, tiles, update, out):
    slot = pl.program_id(0)
    low = lower_half((FINE, 2 * BLOCK))
    owners = [col_owner[place[1] * 16 + j] * 2 for j in range(16)]
    for i in range(16):
        p = row_owner[place[0] * 32 + slot * 16 + i]
        for j in range(0, 16, 2):
            one = tiles[p // 2, owners[j] + p % 2]
            two = tiles[p // 2, owners[j + 1] + p % 2]
            if j < 8:
                both = jnp.where(low, one, pltpu.roll(two, BLOCK, 1))
            else:
                both = jnp.where(low, pltpu.roll(one, BLOCK, 1), two)
            at = (i, 0, slice(None), pl.ds(j * BLOCK, 2 * BLOCK))
            out[at] = both - update[at]


def axis_split(r, c):
    return r // 2, r % 2, c // 8, (c // 2) % 4, c % 2


def panel_kernel(panels, stored, h_ref, row_owner, col_owner, near, update, factor,
                 zs, cs, cp, xs, work, a_blk, b_blk, inv, corner_h, s_buf, h_buf,
                 rh, rl, lh, ll, f_buf, u_buf,
                 own_sem, p1a, p1a_got, p1x, p1x_got, p1c, p1c_got, sends, gets,
                 sib_a, sib_a_got, sib_c, sib_c_got, h_sent, h_got, out_sem):
    r, c = lax.axis_index("row"), lax.axis_index("col")
    x, yl, yh, z, core = axis_split(r, c)

    def col_of(yh_, z_, core_):
        return yh_ * 8 + (z_ % 4) * 2 + core_

    def row_of(x_, yl_):
        return (x_ % 4) * 2 + yl_

    open_sends = []

    def send(src, dst, ss, rs, to):
        copy = pltpu.make_async_remote_copy(
            src_ref=src, dst_ref=dst, send_sem=ss, recv_sem=rs, device_id=to,
            device_id_type=pl.DeviceIdType.MESH,
        )
        copy.start()
        open_sends.append(copy)

    def arrived(ref, sem):
        pltpu.make_async_copy(ref, ref, sem).wait()

    own = [
        pltpu.make_async_copy(stored.at[pl.ds(2 * r, 2)], zs.at[c, r], own_sem.at[0]),
        pltpu.make_async_copy(stored.at[c], xs.at[r, c], own_sem.at[1]),
        pltpu.make_async_copy(stored.at[0], cp.at[core, r], own_sem.at[2]),
    ]
    for copy in own:
        copy.start()
    for d in range(1, 8):
        to = (r + d) % 8
        send(panels.at[pl.ds(2 * to, 2)], zs.at[c, r], p1a.at[d], p1a_got.at[d], (to, c))
    for d in range(1, 16):
        to = (c + d) % 16
        send(panels.at[to], xs.at[r, c], p1x.at[d], p1x_got.at[d], (r, to))
    for d in range(1, 8):
        send(panels.at[0], cp.at[core, r], p1c.at[d], p1c_got.at[d], ((r + d) % 8, c))

    def h_tile(i, j):
        rows = pl.ds(pl.multiple_of(i * 128, 128), 128)
        return h_ref.at[rows, pl.ds(pl.multiple_of(j * 128, 128), 128)]

    def send_tile(n, carry):
        m = n * (45 + 38 * core) % 128
        i = row_of(x + m % 4, (yl + m // 4) % 2)
        j = col_of((2 * yh + yl + m // 4) // 2 % 2, z + m // 16, (core + m // 64) % 2)
        pltpu.make_async_remote_copy(
            src_ref=h_tile(i, j), dst_ref=near.at[r * 16 + c], send_sem=h_sent, recv_sem=h_got,
            device_id=(i, j), device_id_type=pl.DeviceIdType.MESH,
        ).start()
        return carry

    lax.fori_loop(1, EARLY, send_tile, 0)

    zp, zm = (r, col_of(yh, z + 1, core)), (r, col_of(yh, z + 3, core))
    yp, sib = (r, col_of(1 - yh, z, core)), (r, col_of(yh, z, 1 - core))
    xp, xm, lp = (row_of(x + 1, yl), c), (row_of(x + 3, yl), c), (row_of(x, 1 - yl), c)

    def ring(ref, base, index, side, ahead, behind):
        half = ref.shape[1] // 2
        first = lambda k: ref.at[k, pl.ds(0, half)]
        second = lambda k: ref.at[k, pl.ds(half, half)]

        def out(piece, i, to):
            send(piece, piece, sends.at[base + i], gets.at[base + i], to)

        def start():
            mine = index(0, 0)
            out(ref.at[mine], 0, side)
            out(ref.at[mine], 1, ahead)
            out(ref.at[mine], 2, behind)

        def onward(plane):
            i = 1 + 4 * plane
            arrived(ref.at[index(plane, 3)], gets.at[base + i])
            out(first(index(plane, 3)), i + 2, ahead)
            arrived(ref.at[index(plane, 1)], gets.at[base + i + 1])
            out(second(index(plane, 1)), i + 3, behind)

        def beside():
            other = index(1, 0)
            arrived(ref.at[other], gets.at[base])
            out(ref.at[other], 5, ahead)
            out(ref.at[other], 6, behind)

        def last(plane):
            i = 3 + 4 * plane
            arrived(first(index(plane, 2)), gets.at[base + i])
            arrived(second(index(plane, 2)), gets.at[base + i + 1])

        return start, onward, beside, last

    def col_index(plane, d):
        return col_of(yh if plane == 0 else 1 - yh, z + d, core)

    def row_index(plane, d):
        return row_of(x + d, yl if plane == 0 else 1 - yl)

    start_a, onward_a, beside_a, last_a = ring(zs, 0, col_index, yp, zp, zm)
    start_x, onward_x, beside_x, last_x = ring(xs, 9, row_index, lp, xp, xm)
    start_c, onward_c, beside_c, last_c = ring(cs, 18, col_index, yp, zp, zm)
    shares = [(0, 0), (0, 3), (0, 1), (1, 0), (1, 3), (1, 1), (0, 2), (1, 2)]

    def share(ref, ss, rs, i):
        piece = ref.at[col_index(*shares[i])]
        send(piece, piece, ss.at[i], rs.at[i], sib)

    def shared(ref, rs, i):
        plane, d = shares[i]
        arrived(ref.at[col_of(yh if plane == 0 else 1 - yh, z + d, 1 - core)], rs.at[i])

    own[0].wait()
    for d in range(1, 8):
        arrived(zs.at[c, (r + 8 - d) % 8], p1a_got.at[d])
    start_a()
    own[1].wait()
    for d in range(1, 16):
        arrived(xs.at[r, (c + 16 - d) % 16], p1x_got.at[d])
    start_x()
    own[2].wait()
    for d in range(1, 8):
        arrived(cp.at[core, (r + 8 - d) % 8], p1c_got.at[d])
    send(cp.at[core], cp.at[core], p1c.at[0], p1c_got.at[0], sib)
    arrived(cp.at[1 - core], p1c_got.at[0])
    for i in range(4):
        p = row_owner[4 * core + i]
        cs[c, i] = cp[p % 2, p // 2]
    share(zs, sib_a, sib_a_got, 0)
    start_c()
    share(cs, sib_c, sib_c_got, 0)
    onward_a(0)
    onward_x(0)
    beside_a()
    beside_x()
    onward_c(0)
    beside_c()
    for i in range(1, 4):
        share(zs, sib_a, sib_a_got, i)
        share(cs, sib_c, sib_c_got, i)
    onward_a(1)
    onward_x(1)
    onward_c(1)
    for i in range(4, 6):
        share(cs, sib_c, sib_c_got, i)
        share(zs, sib_a, sib_a_got, i)
    last_a(0)
    share(zs, sib_a, sib_a_got, 6)
    last_c(0)
    share(cs, sib_c, sib_c_got, 6)
    last_c(1)
    share(cs, sib_c, sib_c_got, 7)
    last_a(1)
    share(zs, sib_a, sib_a_got, 7)
    lax.fori_loop(EARLY, 128, send_tile, 0)
    kept = pltpu.make_async_copy(h_tile(r, c), near.at[r * 16 + c], h_got)
    kept.start()
    for plane in range(2):
        last_x(plane)
    for i in range(8):
        shared(cs, sib_c_got, i)
    for i in range(8):
        shared(zs, sib_a_got, i)

    fetch_panel(
        lambda i, p, q: cs[2 * q + i // 4, i % 4],
        PANEL // BLOCK, 0, row_owner, col_owner, s_buf, corner_h,
    )
    corner_inverse(s_buf, work, a_blk, b_blk, inv)

    def strip_step(t, carry):
        fetch_panel(
            lambda i, p, q: xs[p // 2, 2 * q + p % 2],
            TALL // BLOCK, c * 16 + t * 4, row_owner, col_owner, s_buf, h_buf,
        )
        special = jnp.logical_and(c == 0, t < 2)
        _, coupling = coupling_of(s_buf[:TALL, :], inv, special, t)
        rest = h_buf[...] - dot(coupling, corner_h[...], 1, 0, HIGHEST)
        at = pl.ds(pl.multiple_of(t * TALL, TALL), TALL)
        rh[at, :PANEL], rl[at, :PANEL] = halves(rest)
        rh[at, PANEL:], rl[at, PANEL:] = halves(coupling)
        return carry

    lax.fori_loop(0, rh.shape[0] // TALL, strip_step, 0)

    def rows_of(t):
        return pl.ds(pl.multiple_of(t * TALL, TALL), TALL)

    def band_step(t, carry):
        slot = t // 4
        fetch_panel(
            lambda i, p, q: zs[2 * q + p % 2, p // 2, slot],
            TALL // BLOCK, r * 32 + t * 4, row_owner, col_owner, s_buf, h_buf,
        )
        special = jnp.logical_and(r == 0, t < 2)
        panel, coupling = coupling_of(s_buf[:TALL, :], inv, special, t)
        f_buf[rows_of(t), :] = panel
        lh[:, :PANEL], ll[:, :PANEL] = halves(coupling)
        lh[:, PANEL:], ll[:, PANEL:] = halves(h_buf[...])
        total = dot(lh[...], rh[...], 1, 1)
        total = total + dot(lh[...], rl[...], 1, 1)
        u_buf[rows_of(t), :] = total + dot(ll[...], rh[...], 1, 1)
        pltpu.make_async_copy(u_buf.at[rows_of(t)], update.at[rows_of(t)], out_sem.at[0, t]).start()
        pltpu.make_async_copy(f_buf.at[rows_of(t)], factor.at[rows_of(t)], out_sem.at[1, t]).start()
        return carry

    steps = u_buf.shape[0] // TALL
    lax.fori_loop(0, steps, band_step, 0)
    for t in range(steps):
        pltpu.make_async_copy(u_buf.at[rows_of(t)], update.at[rows_of(t)], out_sem.at[0, t]).wait()
        pltpu.make_async_copy(f_buf.at[rows_of(t)], factor.at[rows_of(t)], out_sem.at[1, t]).wait()
    arrived(near, h_got)
    arrived(near.at[pl.ds(0, 127)], h_sent)
    for copy in open_sends:
        copy.wait_send()


SMEM = pl.BlockSpec(memory_space=pltpu.SMEM)


def shape_of(shape, dtype=F32):
    return jax.ShapeDtypeStruct(shape, dtype)


def per_device(h_old, s_old, row_owner, col_owner):
    rows_n = lax.axis_size("row")
    cols_n = lax.axis_size("col")
    row_id = lax.axis_index("row")
    col_id = lax.axis_index("col")
    place = jnp.stack([row_id, col_id]).astype(jnp.int32)
    local_h = h_old[0, 0]
    local_s = s_old[0, 0]
    band = ORDER // rows_n
    strip = ORDER // cols_n
    panels = jnp.concatenate([local_s, local_h[:, :BLOCK]], axis=1).reshape(16, BLOCK, 128)
    any_space = pl.BlockSpec(memory_space=pl.ANY)
    dma = pltpu.SemaphoreType.DMA
    vmem = pltpu.VMEM
    near, update, factor = pl.pallas_call(
        panel_kernel,
        out_shape=(shape_of((128, 128, 128)), shape_of((band, strip)), shape_of((band, PANEL))),
        in_specs=[pl.BlockSpec(memory_space=pltpu.VMEM), any_space, any_space, SMEM, SMEM],
        out_specs=(any_space,) * 3,
        scratch_shapes=[
            vmem((16, 8, 2, BLOCK, 128), F32),
            vmem((16, 4, BLOCK, 128), F32),
            vmem((2, 8, BLOCK, 128), F32),
            vmem((8, 16, BLOCK, 128), F32),
            vmem((PANEL // STEP, STEP, 2 * PANEL), F32),
            vmem((STEP, STEP), F32),
            vmem((STEP, STEP), F32),
            vmem((PANEL, PANEL), F32),
            vmem((PANEL, PANEL), F32),
            vmem((PANEL, PANEL), F32),
            vmem((TALL, PANEL), F32),
            vmem((strip, 2 * PANEL), BF16),
            vmem((strip, 2 * PANEL), BF16),
            vmem((TALL, 2 * PANEL), BF16),
            vmem((TALL, 2 * PANEL), BF16),
            vmem((band, PANEL), F32),
            vmem((band, strip), F32),
            dma((3,)), dma((8,)), dma((8,)), dma((16,)), dma((16,)), dma((8,)), dma((8,)),
            dma((27,)), dma((27,)), dma((8,)), dma((8,)), dma((8,)), dma((8,)), dma, dma,
            dma((2, band // TALL)),
        ],
        compiler_params=pltpu.CompilerParams(has_side_effects=True, vmem_limit_bytes=60 * 2**20),
        cost_estimate=pl.CostEstimate(flops=4 * 10**10, bytes_accessed=64 * 2**20, transcendentals=0),
        name="panel",
    )(panels, panels, local_h, row_owner, col_owner)
    h_tiles = near.reshape(rows_n, cols_n, 128, 128)

    fine = pl.BlockSpec((16, 1, FINE, strip), lambda s, u: (s, u, 0, 0))
    h_block = pl.pallas_call(
        final_kernel,
        grid=(2, BLOCK // FINE),
        out_shape=shape_of((band // BLOCK, BLOCK // FINE, FINE, strip)),
        in_specs=[
            SMEM, SMEM, SMEM,
            pl.BlockSpec((rows_n, cols_n, FINE, 128), lambda s, u: (0, 0, s * (BLOCK // FINE) + u, 0)),
            fine,
        ],
        out_specs=fine,
        compiler_params=pltpu.CompilerParams(vmem_limit_bytes=60 * 2**20),
        cost_estimate=pl.CostEstimate(flops=2**22, bytes_accessed=24 * 2**20, transcendentals=0),
        name="final",
    )(place, row_owner, col_owner, h_tiles, update.reshape(band // BLOCK, BLOCK // FINE, FINE, strip))
    return h_block.reshape(band, strip), factor


def solution(mesh):
    in_specs = (P("row", "col", None, None), P("row", "col", None, None), P(), P())
    out_specs = (P("row", "col"), P("row", None))
    return jax.shard_map(
        per_device, mesh=mesh, in_specs=in_specs, out_specs=out_specs, check_vma=False
    )
```
